128 devices in a mesh: prompt: 16 (over z, x_lo, core), ctx: 8 (over x_hi, y).
Axes of the slice: x: 4 (x_hi: 2, x_lo: 2; x = x_hi * 2 + x_lo), y: 4, z: 4, core: 2. Of those that a mesh axis runs over, the one named last changes fastest.
Arguments:
- queries: bfloat16 [65536, 16, 128], P(('prompt', 'ctx')), may hold values from -8 to 8
- keys: bfloat16 [65536, 4, 128], P(('prompt', 'ctx')), may hold values from -8 to 8
- values: bfloat16 [65536, 4, 128], P(('prompt', 'ctx')), may hold values from -6 to 6
- spans: int32 [16, 2], P('prompt'), may hold values from 1 to 3072, as said below
- partner: int32 [16], replicated, may hold values from 0 to 15, each once
Outputs:
- attended: bfloat16 [65536, 16, 128], P(('prompt', 'ctx'))
- decode_cache: bfloat16 [16, 2, 16, 8, 128, 128], P('ctx', None, 'prompt')
The draws below stay inside these ranges and needn't reach their ends.
Inputs may be any that keep to these rules, and one draw needn't show every extreme that they name: `spans`: column 0 counts the image tokens of a prompt, from 1024 to 2048, which come first; column 1 counts the text tokens after them, 1 or more; the two sum to at most 4096, and to exactly 4096 for at least one prompt.
All inputs are finite; a program needn't handle non-finite values.
Results may differ from the reference program's by a relative error of at most 0.0041.
Values may be sent and summed in bfloat16 or wider, within the bound.
No kernel may reach another device: no remote copies, remote signals or barrier semaphores. Data moves between devices by JAX's collectives and lax.ppermute only.
A program may use at most 64 MiB of HBM per device.

```python
import math
import jax
import jax.numpy as jnp
from jax import lax

HEADS = 16
KVH = 4
HD = 128
SEQ = 4096
PROMPTS = 16
TOKENS = 65536
STRIPES = 4
BLOCKS = 8
ROWS_STRIPE = 128


def draw_queries(key, part):
    drawn = jnp.clip(jax.random.normal(jax.random.fold_in(key, 11), (TOKENS, HEADS, HD), jnp.float32), -4.0, 4.0)
    return drawn.astype(jnp.bfloat16)


def draw_keys(key, part):
    drawn = jnp.clip(jax.random.normal(jax.random.fold_in(key, 21), (TOKENS, KVH, HD), jnp.float32), -4.0, 4.0)
    return drawn.astype(jnp.bfloat16)


def draw_spans(key, part):
    image_count = jax.random.randint(jax.random.fold_in(key, 31), (PROMPTS,), SEQ // 4, SEQ // 2 + 1)
    text_count = jax.random.randint(jax.random.fold_in(key, 32), (PROMPTS,), 1, SEQ - image_count + 1)
    fullest = jax.random.randint(jax.random.fold_in(key, 33), (), 0, PROMPTS)
    shortest = (fullest + 1) % PROMPTS
    index_row = jnp.arange(PROMPTS)
    image_count = jnp.where(index_row == fullest, SEQ // 4, image_count)
    text_count = jnp.where(index_row == fullest, SEQ - SEQ // 4, text_count)
    text_count = jnp.where(index_row == shortest, 1, text_count)
    return jnp.stack([image_count, text_count], axis=1).astype(jnp.int32)


def levels(key, dims, split, smallest, top_value):
    def one(position, parts):
        draws = jax.random.uniform(jax.random.fold_in(jax.random.fold_in(key, 6), position), (parts,), jnp.float32, smallest / len(split), top_value / len(split))
        return jnp.repeat(jnp.exp(draws), dims[position] // parts).reshape((-1,) + (1,) * (len(dims) - position - 1))

    gain = one(*split[0])
    for cut in split[1:]:
        gain = gain * one(*cut)
    return gain


def scatter_about(stream_key, dims, scale, most, cuts=(), kind=jnp.bfloat16):
    values = scale * jax.random.normal(stream_key, dims, jnp.float32)
    if cuts:
        values = values * levels(stream_key, dims, cuts, -0.22, 0.18)
    return jnp.clip(values, -most, most).astype(kind)


def setup_inputs(seed: int = 0) -> dict:
    key_list = jax.random.split(jax.random.key(seed), 6)
    return {
        "queries": draw_queries(jax.random.fold_in(key_list[5], 71), 0),
        "keys": draw_keys(jax.random.fold_in(key_list[5], 71), 0),
        "values": scatter_about(key_list[2], (TOKENS, KVH, HD), 1.0, 6.0, ((0, 128),)),
        "spans": draw_spans(jax.random.fold_in(key_list[5], 71), 0),
        "partner": jax.random.permutation(key_list[4], PROMPTS).astype(jnp.int32),
    }


def attend_prompt(prompt_item):
    prompt_queries, prompt_keys, prompt_values, length = prompt_item
    qblock = math.gcd(SEQ, 512)
    block_count = SEQ // qblock
    members = HEADS // KVH
    grouped = prompt_queries.reshape(block_count, qblock, KVH, members, HD)
    keys_wide = prompt_keys.astype(jnp.float32)
    values_wide = prompt_values.astype(jnp.float32)
    key_pos = lax.iota(jnp.int32, SEQ)

    def one_block(block_item):
        query_block, block_index = block_item
        query_pos = block_index * qblock + lax.iota(jnp.int32, qblock)
        scores = jnp.einsum('qgmd,kgd->qgmk', query_block.astype(jnp.float32), keys_wide) * (1.0 / math.sqrt(HD))
        allowed = ((key_pos[None, :] <= query_pos[:, None]) & (key_pos[None, :] < length))[:, None, None, :]
        scores = jnp.where(allowed, scores, -1e+30)
        row_peak = lax.optimization_barrier(jnp.max(scores, axis=-1, keepdims=True))
        weights = jnp.where(allowed, jnp.exp(scores - row_peak), 0.0)
        rounded = lax.optimization_barrier(weights.astype(jnp.bfloat16)).astype(jnp.float32)
        mixture = jnp.einsum('qgmk,kgd->qgmd', rounded, values_wide) / lax.optimization_barrier(jnp.sum(weights, axis=-1))[..., None]
        mixture = jnp.where((query_pos < length)[:, None, None, None], mixture, 0.0)
        return mixture.reshape(qblock, HEADS, HD).astype(jnp.bfloat16)
    finished = lax.map(one_block, (grouped, jnp.arange(block_count, dtype=jnp.int32)))
    return finished.reshape(SEQ, HEADS, HD)

def reference(queries, keys, values, spans, partner):
    lengths = spans[:, 0] + spans[:, 1]
    prompt_queries = queries.reshape(PROMPTS, SEQ, HEADS, HD)
    prompt_keys = keys.reshape(PROMPTS, SEQ, KVH, HD)
    prompt_values = values.reshape(PROMPTS, SEQ, KVH, HD)
    attended = lax.map(attend_prompt, (prompt_queries, prompt_keys, prompt_values, lengths))
    attended = attended.reshape(TOKENS, HEADS, HD)
    live_rows = (lax.iota(jnp.int32, SEQ)[None, :] < lengths[:, None])[:, :, None, None]
    paired = jnp.stack([jnp.where(live_rows, prompt_keys, jnp.zeros_like(prompt_keys)), jnp.where(live_rows, prompt_values, jnp.zeros_like(prompt_values))], axis=1)
    paired = jnp.take(paired, partner.astype(jnp.int32), axis=0)
    paired = paired.reshape(PROMPTS, 2, BLOCKS, ROWS_STRIPE, STRIPES, KVH, HD)
    decode_cache = paired.transpose(0, 1, 4, 5, 2, 3, 6).reshape(PROMPTS, 2, STRIPES * KVH, BLOCKS, ROWS_STRIPE, HD)
    return (attended, decode_cache)
```

```python
import math

import jax
import jax.numpy as jnp
from jax import lax
from jax.experimental import pallas as pl
from jax.experimental.pallas import tpu as pltpu
from jax.sharding import PartitionSpec as P

far_below = -1e30


def attend(got, heads, length):
    blocks, planes, rows, width = got.shape
    columns = heads * rows
    half = columns // 2
    log2_scale = 1.4426950408889634 / math.sqrt(width)

    def kernel(length_ref, q_ref, kv_ref, o_ref, values_t, query_t, mixed, peak, total, held):
        block = pl.program_id(0)
        live = length_ref[0]

        @pl.when(block == 0)
        def _():
            for j in range(blocks):
                values_t[:, j * rows : (j + 1) * rows] = kv_ref[j, 1].T

        @pl.when(block * rows >= live)
        def _():
            o_ref[...] = jnp.zeros_like(o_ref)

        @pl.when(block * rows < live)
        def _():
            for h in range(heads):
                query_t[:, h * rows : (h + 1) * rows] = q_ref[0, h].T
            mixed[...] = jnp.zeros_like(mixed)
            peak[...] = jnp.full_like(peak, far_below)
            total[...] = jnp.zeros_like(total)

            def scores(j, part):
                return jnp.dot(kv_ref[j, 0], query_t[:, part], preferred_element_type=jnp.float32)

            def fold(s, j, part):
                value_block = values_t[:, pl.ds(pl.multiple_of(j * rows, rows), rows)]
                old = peak[:, part]
                new = jnp.maximum(old, jnp.max(s, axis=0, keepdims=True))
                weights = jnp.exp2((s - new) * log2_scale)
                factor = jnp.exp2((old - new) * log2_scale)
                total[:, part] = total[:, part] * factor + jnp.sum(weights, axis=0, keepdims=True)
                mixed[:, part] = mixed[:, part] * factor + jnp.dot(
                    value_block, weights.astype(jnp.bfloat16), preferred_element_type=jnp.float32
                )
                peak[:, part] = new

            parts = [slice(a, a + half) for a in range(0, columns, half)]

            def earlier(slot, j):
                for part in parts:
                    s = held[slot, :, part]
                    held[1 - slot, :, part] = scores(j + 1, part)
                    fold(s, j, part)

            def diagonal(slot):
                for part in parts:
                    key_pos = lax.broadcasted_iota(jnp.int32, (rows, half), 0)
                    query_pos = lax.broadcasted_iota(jnp.int32, (rows, half), 1) + part.start
                    allowed = key_pos <= lax.rem(query_pos, rows)
                    fold(jnp.where(allowed, held[slot, :, part], far_below), block, part)

            for part in parts:
                held[0, :, part] = scores(0, part)

            def two(t, carry):
                earlier(0, 2 * t)
                earlier(1, 2 * t + 1)
                return carry

            lax.fori_loop(0, block // 2, two, 0)

            @pl.when(lax.rem(block, 2) == 1)
            def _():
                earlier(0, block - 1)
                diagonal(1)

            @pl.when(lax.rem(block, 2) == 0)
            def _():
                diagonal(0)

            position = block * rows + lax.broadcasted_iota(jnp.int32, (rows, 1), 0)
            for h in range(heads):
                part = slice(h * rows, (h + 1) * rows)
                mixture = (mixed[:, part] / total[:, part]).T
                o_ref[0, h] = jnp.where(position < live, mixture, 0.0).astype(jnp.bfloat16)

    return pl.pallas_call(
        kernel,
        grid_spec=pltpu.PrefetchScalarGridSpec(
            num_scalar_prefetch=1,
            grid=(blocks,),
            in_specs=[
                pl.BlockSpec((1, heads, rows, width), lambda i, n: (i, 0, 0, 0)),
                pl.BlockSpec((blocks, 2, rows, width), lambda i, n: (0, heads // 2, 0, 0)),
            ],
            out_specs=pl.BlockSpec((1, heads, rows, width), lambda i, n: (i, 0, 0, 0)),
            scratch_shapes=[
                pltpu.VMEM((width, blocks * rows), jnp.bfloat16),
                pltpu.VMEM((width, columns), jnp.bfloat16),
                pltpu.VMEM((width, columns), jnp.float32),
                pltpu.VMEM((1, columns), jnp.float32),
                pltpu.VMEM((1, columns), jnp.float32),
                pltpu.VMEM((2, rows, columns), jnp.float32),
            ],
        ),
        out_shape=jax.ShapeDtypeStruct((blocks, heads, rows, width), jnp.bfloat16),
        compiler_params=pltpu.CompilerParams(dimension_semantics=("arbitrary",)),
        cost_estimate=pl.CostEstimate(
            flops=2 * blocks * blocks * heads * rows * rows * width,
            bytes_accessed=2 * blocks * rows * width * (2 * heads + 2),
            transcendentals=blocks * blocks * rows * rows * heads // 2,
        ),
    )(length, got, got)


def take_blocks(array, order):
    block = (1,) + array.shape[1:]

    def kernel(order_ref, in_ref, out_ref):
        out_ref[...] = in_ref[...]

    return pl.pallas_call(
        kernel,
        grid_spec=pltpu.PrefetchScalarGridSpec(
            num_scalar_prefetch=1,
            grid=(array.shape[0],),
            in_specs=[pl.BlockSpec(block, lambda i, order_ref: (order_ref[i], 0, 0, 0))],
            out_specs=pl.BlockSpec(block, lambda i, order_ref: (i, 0, 0, 0)),
        ),
        out_shape=jax.ShapeDtypeStruct(array.shape, array.dtype),
    )(order, array)


def swap(array, axis):
    return lax.all_to_all(array, axis, split_axis=0, concat_axis=0, tiled=True)


def per_device(queries, keys, values, spans, partner):
    rows, head_count, width = queries.shape
    kv_heads = keys.shape[1]
    blocks = lax.axis_size("ctx")
    slots = lax.axis_size("prompt")
    stripes = slots // kv_heads
    share = head_count // blocks
    copies = blocks // kv_heads
    length = spans[0, 0] + spans[0, 1]

    pair = jnp.stack([keys, values])
    by_head = jnp.repeat(pair.transpose(2, 0, 1, 3), copies, axis=0)
    q_by_head = queries.transpose(1, 0, 2).reshape(blocks, share, rows, width)
    sent = jnp.concatenate([q_by_head, by_head], axis=1)
    got = swap(sent, "ctx")

    first = lax.axis_index("ctx") * rows
    live = (first + lax.iota(jnp.int32, rows) < length)[None, :, None, None]
    kept, got = lax.optimization_barrier((pair, got))
    slot_rows = jnp.where(live, kept, jnp.zeros_like(kept))
    slot_rows = slot_rows.reshape(2, rows // stripes, stripes * kv_heads, width).transpose(2, 0, 1, 3)
    by_prompt = swap(slot_rows, "prompt")

    finished = attend(got, share, length[None])
    by_row = take_blocks(by_prompt, partner)
    cache = swap(by_row, "ctx")
    held_rows = slots // blocks
    cache = cache.reshape(blocks, held_rows, 2, rows // stripes, width).transpose(1, 2, 0, 3, 4)
    cache = cache[:, :, None]

    back = swap(finished, "ctx")
    attended = back.reshape(head_count, rows, width).transpose(1, 0, 2)
    return attended, cache


def solution(mesh):
    placed = P(("prompt", "ctx"), None, None)
    return jax.shard_map(
        per_device,
        mesh=mesh,
        in_specs=(placed, placed, placed, P("prompt", None), P()),
        out_specs=(placed, P("ctx", None, "prompt", None, None, None)),
        check_vma=False,
    )
```

```python
import math

import jax
import jax.numpy as jnp
from jax import lax
from jax.experimental import pallas as pl
from jax.experimental.pallas import tpu as pltpu
from jax.sharding import PartitionSpec as P

far_below = -1e30
groups = [[0, 3, 4, 7], [1, 2, 5, 6]]


def attend(queries, own, other, scalars):
    members, heads, rows, width = queries.shape
    columns = heads * rows
    part_size = min(columns, 512)
    blocks = 2 * members
    log2_scale = 1.4426950408889634 / math.sqrt(width)

    def kernel(scalar_ref, q_ref, own_ref, other_ref, o_ref, key_blocks, values_t, query_t, mixed, peak, total, held):
        step = pl.program_id(0)
        live = scalar_ref[0]
        block = scalar_ref[1 + step]

        @pl.when(step == 0)
        def _():
            for source, at in ((own_ref, 1), (other_ref, 1 + members)):
                for m in range(members):
                    there = scalar_ref[at + m]
                    key_blocks[there] = source[m, 0]
                    values_t[there] = source[m, 1].T

        @pl.when(block * rows >= live)
        def _():
            o_ref[...] = jnp.zeros_like(o_ref)

        @pl.when(block * rows < live)
        def _():
            for h in range(heads):
                query_t[:, h * rows : (h + 1) * rows] = q_ref[0, h].T
            mixed[...] = jnp.zeros_like(mixed)
            peak[...] = jnp.full_like(peak, far_below)
            total[...] = jnp.zeros_like(total)

            def scores(j, part):
                return jnp.dot(key_blocks[j], query_t[:, part], preferred_element_type=jnp.float32)

            def fold(s, j, part):
                old = peak[:, part]
                new = jnp.maximum(old, jnp.max(s, axis=0, keepdims=True))
                weights = jnp.exp2((s - new) * log2_scale)
                factor = jnp.exp2((old - new) * log2_scale)
                total[:, part] = total[:, part] * factor + jnp.sum(weights, axis=0, keepdims=True)
                mixed[:, part] = mixed[:, part] * factor + jnp.dot(
                    values_t[j], weights.astype(jnp.bfloat16), preferred_element_type=jnp.float32
                )
                peak[:, part] = new

            parts = [slice(a, a + part_size) for a in range(0, columns, part_size)]

            def earlier(slot, j):
                for part in parts:
                    s = held[slot, :, part]
                    held[1 - slot, :, part] = scores(j + 1, part)
                    fold(s, j, part)

            def diagonal(slot):
                for part in parts:
                    key_pos = lax.broadcasted_iota(jnp.int32, (rows, part_size), 0)
                    query_pos = lax.broadcasted_iota(jnp.int32, (rows, part_size), 1) + part.start
                    allowed = key_pos <= lax.rem(query_pos, rows)
                    fold(jnp.where(allowed, held[slot, :, part], far_below), block, part)

            for part in parts:
                held[0, :, part] = scores(0, part)

            def two(t, carry):
                earlier(0, 2 * t)
                earlier(1, 2 * t + 1)
                return carry

            lax.fori_loop(0, block // 2, two, 0)

            @pl.when(lax.rem(block, 2) == 1)
            def _():
                earlier(0, block - 1)
                diagonal(1)

            @pl.when(lax.rem(block, 2) == 0)
            def _():
                diagonal(0)

            position = block * rows + lax.broadcasted_iota(jnp.int32, (rows, 1), 0)
            for h in range(heads):
                part = slice(h * rows, (h + 1) * rows)
                mixture = (mixed[:, part] / total[:, part]).T
                o_ref[0, h] = jnp.where(position < live, mixture, 0.0).astype(jnp.bfloat16)

    whole = pl.BlockSpec((members, 2, rows, width), lambda i, n: (0, 0, 0, 0))
    return pl.pallas_call(
        kernel,
        grid_spec=pltpu.PrefetchScalarGridSpec(
            num_scalar_prefetch=1,
            grid=(members,),
            in_specs=[
                pl.BlockSpec((1, heads, rows, width), lambda i, n: (i, 0, 0, 0)),
                whole,
                whole,
            ],
            out_specs=pl.BlockSpec((1, heads, rows, width), lambda i, n: (i, 0, 0, 0)),
            scratch_shapes=[
                pltpu.VMEM((blocks, rows, width), jnp.bfloat16),
                pltpu.VMEM((blocks, width, rows), jnp.bfloat16),
                pltpu.VMEM((width, columns), jnp.bfloat16),
                pltpu.VMEM((width, columns), jnp.float32),
                pltpu.VMEM((1, columns), jnp.float32),
                pltpu.VMEM((1, columns), jnp.float32),
                pltpu.VMEM((2, rows, columns), jnp.float32),
            ],
        ),
        out_shape=jax.ShapeDtypeStruct(queries.shape, jnp.bfloat16),
        compiler_params=pltpu.CompilerParams(
            dimension_semantics=("arbitrary",), vmem_limit_bytes=40 * 1024 * 1024
        ),
        cost_estimate=pl.CostEstimate(
            flops=4 * members * members * heads * rows * rows * width,
            bytes_accessed=4 * members * rows * width * (heads + 2),
            transcendentals=members * members * rows * rows * heads,
        ),
    )(scalars, queries, own, other)


def take_blocks(array, order):
    block = (1,) + array.shape[1:]

    def kernel(order_ref, in_ref, out_ref):
        out_ref[...] = in_ref[...]

    return pl.pallas_call(
        kernel,
        grid_spec=pltpu.PrefetchScalarGridSpec(
            num_scalar_prefetch=1,
            grid=(array.shape[0],),
            in_specs=[pl.BlockSpec(block, lambda i, order_ref: (order_ref[i], 0, 0, 0))],
            out_specs=pl.BlockSpec(block, lambda i, order_ref: (i, 0, 0, 0)),
        ),
        out_shape=jax.ShapeDtypeStruct(array.shape, array.dtype),
        compiler_params=pltpu.CompilerParams(vmem_limit_bytes=8 * 1024 * 1024),
    )(order, array)


def swap(array, axis, index_groups=None):
    return lax.all_to_all(
        array, axis, split_axis=0, concat_axis=0, axis_index_groups=index_groups, tiled=True
    )


def per_device(queries, keys, values, spans, partner):
    rows, head_count, width = queries.shape
    kv_heads = keys.shape[1]
    blocks = lax.axis_size("ctx")
    slots = lax.axis_size("prompt")
    stripes = slots // kv_heads
    length = spans[0, 0] + spans[0, 1]
    ctx = lax.axis_index("ctx")

    pair = jnp.stack([keys, values])
    own = swap(pair.transpose(2, 0, 1, 3), "ctx", groups)
    by_head = queries.transpose(1, 0, 2).reshape(kv_heads, head_count // kv_heads, rows, width)
    q_own = swap(by_head, "ctx", groups)
    facing = list(zip(groups[0] + groups[1], groups[1] + groups[0]))
    other = lax.ppermute(own, "ctx", facing)

    live = (ctx * rows + lax.iota(jnp.int32, rows) < length)[None, :, None, None]
    slot_rows = jnp.where(live, pair, jnp.zeros_like(pair))
    slot_rows = slot_rows.reshape(2, rows // stripes, slots, width).transpose(2, 0, 1, 3)
    slot_rows, other, q_own = lax.optimization_barrier((slot_rows, other, q_own))
    by_prompt = swap(slot_rows, "prompt")

    places = jnp.array(groups, jnp.int32)
    first = (ctx % 4 == 0) | (ctx % 4 == 3)
    mine = jnp.where(first, places[0], places[1])
    theirs = jnp.where(first, places[1], places[0])
    scalars = jnp.concatenate([length[None], mine, theirs])
    finished = attend(q_own, own, other, scalars)
    back = swap(finished, "ctx", groups)
    attended = back.reshape(head_count, rows, width).transpose(1, 0, 2)

    by_row = take_blocks(by_prompt, partner)
    cache = swap(by_row, "ctx")
    held_rows = slots // blocks
    cache = cache.reshape(blocks, held_rows, 2, rows // stripes, width).transpose(1, 2, 0, 3, 4)
    return attended, cache[:, :, None]


def solution(mesh):
    placed = P(("prompt", "ctx"), None, None)
    return jax.shard_map(
        per_device,
        mesh=mesh,
        in_specs=(placed, placed, placed, P("prompt", None), P()),
        out_specs=(placed, P("ctx", None, "prompt", None, None, None)),
        check_vma=False,
    )
```

```python
import math

import jax
import jax.numpy as jnp
from jax import lax
from jax.experimental import pallas as pl
from jax.experimental.pallas import tpu as pltpu
from jax.sharding import PartitionSpec as P

far_below = -1e30


def partner_of(k, c):
    across = c % 4
    across = 3 - across if k & 1 else across
    x = c // 4
    x = 1 - x if k & 2 else x
    return 4 * x + across


def facing(c):
    return c - c % 2 + (1 - c % 2)


def route(relation):
    return [(c, relation(c)) for c in range(8)]


def small(limit):
    return pltpu.CompilerParams(vmem_limit_bytes=limit * 1024 * 1024)


def vmem_specs(count):
    return [pl.BlockSpec(memory_space=pltpu.VMEM)] * count


def pack_kv(keys, values, scalars, kv_heads):
    short, slots, width = keys.shape
    stripes = slots // kv_heads
    rows = short * stripes

    def kernel(scalar_ref, k_ref, v_ref, *refs):
        outs, slot_ref, turned = refs[:4], refs[4], refs[5]
        group, first, live = scalar_ref[0], scalar_ref[1], scalar_ref[2]
        for t, ref in enumerate((k_ref, v_ref)):
            turned[t] = jnp.swapaxes(ref[...], 0, 1)
        for k in range(4):
            for t in range(2):
                for stripe in range(stripes):
                    outs[k][t, stripe * short : (stripe + 1) * short, :] = turned[
                        t, stripe * kv_heads + (group ^ k)
                    ]
        for slot in range(slots):
            position = (
                first + lax.broadcasted_iota(jnp.int32, (short, 1), 0) * stripes + slot // kv_heads
            )
            for t in range(2):
                slot_ref[slot, t] = jnp.where(
                    position < live, turned[t, slot].astype(jnp.float32), 0.0
                ).astype(jnp.bfloat16)

    piece = jax.ShapeDtypeStruct((2, rows, width), jnp.bfloat16)
    return pl.pallas_call(
        kernel,
        in_specs=[pl.BlockSpec(memory_space=pltpu.SMEM)] + vmem_specs(2),
        out_specs=vmem_specs(5),
        out_shape=[piece] * 4 + [jax.ShapeDtypeStruct((slots, 2, short, width), jnp.bfloat16)],
        scratch_shapes=[pltpu.VMEM((2, slots, short, width), jnp.bfloat16)],
        compiler_params=small(12),
    )(scalars, keys, values)


def pack_queries(queries, scalars):
    rows, head_count, width = queries.shape
    heads = head_count // 4

    def kernel(scalar_ref, q_ref, *refs):
        outs, turned = refs[:4], refs[4]
        turned[...] = jnp.swapaxes(q_ref[...], 0, 1)
        for k in range(4):
            outs[k][...] = turned[pl.ds((scalar_ref[0] ^ k) * heads, heads)]

    piece = jax.ShapeDtypeStruct((heads, rows, width), jnp.bfloat16)
    return pl.pallas_call(
        kernel,
        in_specs=[pl.BlockSpec(memory_space=pltpu.SMEM)] + vmem_specs(1),
        out_specs=vmem_specs(4),
        out_shape=[piece] * 4,
        scratch_shapes=[pltpu.VMEM((head_count, rows, width), jnp.bfloat16)],
        compiler_params=small(16),
    )(scalars, queries)


def join_heads(pieces, scalars):
    heads, rows, width = pieces[0].shape

    def kernel(scalar_ref, *refs):
        ins, out, gathered = refs[:4], refs[4], refs[5]
        for k in range(4):
            gathered[pl.ds((scalar_ref[0] ^ k) * heads, heads)] = ins[k][...]
        out[...] = jnp.swapaxes(gathered[...], 0, 1)

    return pl.pallas_call(
        kernel,
        in_specs=[pl.BlockSpec(memory_space=pltpu.SMEM)] + vmem_specs(4),
        out_specs=vmem_specs(1)[0],
        out_shape=jax.ShapeDtypeStruct((rows, 4 * heads, width), jnp.bfloat16),
        scratch_shapes=[pltpu.VMEM((4 * heads, rows, width), jnp.bfloat16)],
        compiler_params=small(16),
    )(scalars, *pieces)


def attend(queries, own, other_first, other_rest, scalars, stripes):
    members = len(queries)
    heads, rows, width = queries[0].shape
    columns = heads * rows
    part_size = min(columns, 512)
    blocks = 2 * members
    log2_scale = 1.4426950408889634 / math.sqrt(width)

    def kernel(scalar_ref, *refs):
        q_refs, own_refs, first_ref, rest_ref = refs[:4], refs[4:8], refs[8], refs[9]
        o_refs = refs[10:14]
        key_blocks, values_t, query_t, mixed, peak, total, held = refs[14:]
        step = pl.program_id(0)
        live = scalar_ref[2]
        block = scalar_ref[3 + step]

        @pl.when(step == 0)
        def _():
            rest = [rest_ref.at[m] for m in range(members - 1)]
            for m, source in enumerate((*own_refs, first_ref, *rest)):
                there = scalar_ref[3 + m]
                key_blocks[there] = source[0]
                values_t[there] = source[1].T

        @pl.when(block * rows >= live)
        def _():
            for m in range(members):

                @pl.when(step == m)
                def _():
                    o_refs[m][...] = jnp.zeros_like(o_refs[m])

        @pl.when(block * rows < live)
        def _():
            for m in range(members):

                @pl.when(step == m)
                def _():
                    for h in range(heads):
                        query_t[:, h * rows : (h + 1) * rows] = q_refs[m][h].T

            mixed[...] = jnp.zeros_like(mixed)
            peak[...] = jnp.full_like(peak, far_below)
            total[...] = jnp.zeros_like(total)

            def scores(j, part):
                return jnp.dot(key_blocks[j], query_t[:, part], preferred_element_type=jnp.float32)

            def fold(s, j, part):
                old = peak[:, part]
                new = jnp.maximum(old, jnp.max(s, axis=0, keepdims=True))
                weights = jnp.exp2((s - new) * log2_scale)
                factor = jnp.exp2((old - new) * log2_scale)
                total[:, part] = total[:, part] * factor + jnp.sum(weights, axis=0, keepdims=True)
                mixed[:, part] = mixed[:, part] * factor + jnp.dot(
                    values_t[j], weights.astype(jnp.bfloat16), preferred_element_type=jnp.float32
                )
                peak[:, part] = new

            parts = [slice(a, a + part_size) for a in range(0, columns, part_size)]

            def earlier(slot, j):
                for part in parts:
                    s = held[slot, :, part]
                    held[1 - slot, :, part] = scores(j + 1, part)
                    fold(s, j, part)

            def diagonal(slot):
                for part in parts:
                    key_row = lax.broadcasted_iota(jnp.int32, (rows, part_size), 0)
                    key_pos = lax.rem(key_row, rows // stripes) * stripes + key_row // (rows // stripes)
                    query_pos = lax.broadcasted_iota(jnp.int32, (rows, part_size), 1) + part.start
                    allowed = key_pos <= lax.rem(query_pos, rows)
                    fold(jnp.where(allowed, held[slot, :, part], far_below), block, part)

            for part in parts:
                held[0, :, part] = scores(0, part)

            def two(t, carry):
                earlier(0, 2 * t)
                earlier(1, 2 * t + 1)
                return carry

            lax.fori_loop(0, block // 2, two, 0)

            @pl.when(lax.rem(block, 2) == 1)
            def _():
                earlier(0, block - 1)
                diagonal(1)

            @pl.when(lax.rem(block, 2) == 0)
            def _():
                diagonal(0)

            position = block * rows + lax.broadcasted_iota(jnp.int32, (rows, 1), 0)
            for h in range(heads):
                part = slice(h * rows, (h + 1) * rows)
                mixture = (mixed[:, part] / total[:, part]).T
                mixture = jnp.where(position < live, mixture, 0.0).astype(jnp.bfloat16)
                for m in range(members):

                    @pl.when(step == m)
                    def _():
                        o_refs[m][h] = mixture

    def whole(shape):
        return pl.BlockSpec(shape, lambda i, n: (0,) * len(shape))

    arrays = (*queries, *own, other_first, other_rest)
    return pl.pallas_call(
        kernel,
        grid_spec=pltpu.PrefetchScalarGridSpec(
            num_scalar_prefetch=1,
            grid=(members,),
            in_specs=[whole(array.shape) for array in arrays],
            out_specs=[whole(queries[0].shape)] * members,
            scratch_shapes=[
                pltpu.VMEM((blocks, rows, width), jnp.bfloat16),
                pltpu.VMEM((blocks, width, rows), jnp.bfloat16),
                pltpu.VMEM((width, columns), jnp.bfloat16),
                pltpu.VMEM((width, columns), jnp.float32),
                pltpu.VMEM((1, columns), jnp.float32),
                pltpu.VMEM((1, columns), jnp.float32),
                pltpu.VMEM((2, rows, columns), jnp.float32),
            ],
        ),
        out_shape=[jax.ShapeDtypeStruct(queries[0].shape, jnp.bfloat16)] * members,
        compiler_params=pltpu.CompilerParams(
            dimension_semantics=("arbitrary",), vmem_limit_bytes=40 * 1024 * 1024
        ),
        cost_estimate=pl.CostEstimate(
            flops=4 * members * members * heads * rows * rows * width,
            bytes_accessed=4 * members * rows * width * (heads + 2),
            transcendentals=members * members * rows * rows * heads,
        ),
    )(scalars, *arrays)


def take_blocks(array, order):
    def kernel(order_ref, in_ref, out_ref):
        for i in range(array.shape[0]):
            out_ref[i] = in_ref[order_ref[i]]

    return pl.pallas_call(
        kernel,
        in_specs=[pl.BlockSpec(memory_space=pltpu.SMEM)] + vmem_specs(1),
        out_specs=vmem_specs(1)[0],
        out_shape=jax.ShapeDtypeStruct(array.shape, array.dtype),
        compiler_params=small(8),
    )(order, array)


def swap(array, axis):
    return lax.all_to_all(array, axis, split_axis=0, concat_axis=0, tiled=True)


def per_device(queries, keys, values, spans, partner):
    rows, head_count, width = queries.shape
    kv_heads = keys.shape[1]
    blocks = lax.axis_size("ctx")
    slots = lax.axis_size("prompt")
    stripes = slots // kv_heads
    length = spans[0, 0] + spans[0, 1]
    ctx = lax.axis_index("ctx")
    places = jnp.array([[partner_of(k, c) for k in range(4)] for c in range(blocks)], jnp.int32)
    facing_places = jnp.array(
        [[partner_of(k, facing(c)) for k in range(4)] for c in range(blocks)], jnp.int32
    )
    scalars = jnp.concatenate(
        [
            jnp.stack([ctx // 2, ctx * rows, length]),
            lax.dynamic_index_in_dim(places, ctx, 0, keepdims=False),
            lax.dynamic_index_in_dim(facing_places, ctx, 0, keepdims=False),
        ]
    )
    routes = [route(lambda c, k=k: partner_of(k, c)) for k in range(4)]

    by_slot = (rows // stripes, slots, width)
    *kv_out, slot_rows = pack_kv(keys.reshape(by_slot), values.reshape(by_slot), scalars, kv_heads)
    own = [kv_out[0]] + [lax.ppermute(kv_out[k], "ctx", routes[k]) for k in (1, 2, 3)]
    other_first = lax.ppermute(kv_out[0], "ctx", route(facing))
    queries, slot_rows, *kv_out = lax.optimization_barrier((queries, slot_rows, *kv_out))
    q_out = pack_queries(queries, scalars)
    q_own = [q_out[0]] + [lax.ppermute(q_out[k], "ctx", routes[k]) for k in (1, 2, 3)]
    other_rest = lax.ppermute(jnp.stack(own[1:]), "ctx", route(facing))

    slot_rows, *q_out = lax.optimization_barrier((slot_rows, *q_out))
    by_prompt = swap(slot_rows, "prompt")
    by_row = take_blocks(by_prompt, partner)
    cache = swap(by_row, "ctx")
    held_rows = slots // blocks
    cache = cache.reshape(blocks, held_rows, 2, rows // stripes, width).transpose(1, 2, 0, 3, 4)

    finished = attend(q_own, own, other_first, other_rest, scalars, stripes)
    back = [finished[0]] + [lax.ppermute(finished[k], "ctx", routes[k]) for k in (1, 2, 3)]
    return join_heads(back, scalars), cache[:, :, None]


def solution(mesh):
    placed = P(("prompt", "ctx"), None, None)
    return jax.shard_map(
        per_device,
        mesh=mesh,
        in_specs=(placed, placed, placed, P("prompt", None), P()),
        out_specs=(placed, P("ctx", None, "prompt", None, None, None)),
        check_vma=False,
    )
```

```python
import math

import jax
import jax.numpy as jnp
from jax import lax
from jax.experimental import pallas as pl
from jax.experimental.pallas import tpu as pltpu
from jax.sharding import PartitionSpec as P

far_below = -1e30


flips = (0, 3, 4, 7)


def route(flip):
    return [(c, c ^ flip) for c in range(8)]


def small(limit):
    return pltpu.CompilerParams(vmem_limit_bytes=limit * 1024 * 1024)


def whole(array):
    return pl.BlockSpec(array.shape, lambda *_: (0,) * len(array.shape))


def pack_kv(keys, values, spans, kv_heads):
    short, slots, width = keys.shape
    stripes = slots // kv_heads
    rows = short * stripes

    def kernel(spans_ref, k_ref, v_ref, *refs):
        outs, slot_ref, turned = refs[:4], refs[4], refs[5]
        ctx = lax.axis_index("ctx")
        group, first = ctx // 2, ctx * rows
        live = spans_ref[0, 0] + spans_ref[0, 1]
        for t, ref in enumerate((k_ref, v_ref)):
            turned[t] = jnp.swapaxes(ref[...], 0, 1)
        for k in range(4):
            for t in range(2):
                for stripe in range(stripes):
                    outs[k][t, stripe * short : (stripe + 1) * short, :] = turned[
                        t, stripe * kv_heads + (group ^ k)
                    ]
        for slot in range(slots):
            position = (
                first + lax.broadcasted_iota(jnp.int32, (short, 1), 0) * stripes + slot // kv_heads
            )
            for t in range(2):
                slot_ref[slot, t] = jnp.where(
                    position < live, turned[t, slot].astype(jnp.float32), 0.0
                ).astype(jnp.bfloat16)

    piece = jax.ShapeDtypeStruct((2, rows, width), jnp.bfloat16)
    out_shape = [piece] * 4 + [jax.ShapeDtypeStruct((slots, 2, short, width), jnp.bfloat16)]
    return pl.pallas_call(
        kernel,
        in_specs=[pl.BlockSpec(memory_space=pltpu.SMEM), whole(keys), whole(values)],
        out_specs=[whole(out) for out in out_shape],
        out_shape=out_shape,
        scratch_shapes=[pltpu.VMEM((2, slots, short, width), jnp.bfloat16)],
        compiler_params=small(12),
    )(spans, keys, values)


def pack_queries(queries):
    rows, head_count, width = queries.shape
    heads = head_count // 4

    def kernel(q_ref, *refs):
        outs, turned = refs[:4], refs[4]
        group = lax.axis_index("ctx") // 2
        turned[...] = jnp.swapaxes(q_ref[...], 0, 1)
        for k in range(4):
            outs[k][...] = turned[pl.ds((group ^ k) * heads, heads)]

    piece = jax.ShapeDtypeStruct((heads, rows, width), jnp.bfloat16)
    return pl.pallas_call(
        kernel,
        in_specs=[whole(queries)],
        out_specs=[whole(piece)] * 4,
        out_shape=[piece] * 4,
        scratch_shapes=[pltpu.VMEM((head_count, rows, width), jnp.bfloat16)],
        compiler_params=small(16),
    )(queries)


def join_heads(pieces):
    heads, rows, width = pieces[0].shape

    def kernel(*refs):
        ins, out, gathered = refs[:4], refs[4], refs[5]
        group = lax.axis_index("ctx") // 2
        for k in range(4):
            gathered[pl.ds((group ^ k) * heads, heads)] = ins[k][...]
        out[...] = jnp.swapaxes(gathered[...], 0, 1)

    out_shape = jax.ShapeDtypeStruct((rows, 4 * heads, width), jnp.bfloat16)
    return pl.pallas_call(
        kernel,
        in_specs=[whole(piece) for piece in pieces],
        out_specs=whole(out_shape),
        out_shape=out_shape,
        scratch_shapes=[pltpu.VMEM((4 * heads, rows, width), jnp.bfloat16)],
        compiler_params=small(16),
    )(*pieces)


def attend(which, queries, own, other_first, other_rest, spans, stripes):
    asked = len(which)
    members = len(own)
    heads, rows, width = queries[0].shape
    columns = heads * rows
    part_size = min(columns, 512)
    blocks = 2 * members
    log2_scale = 1.4426950408889634 / math.sqrt(width)

    def kernel(spans_ref, *refs):
        q_refs, own_refs = refs[:asked], refs[asked : asked + members]
        first_ref, rest_ref, *o_refs = refs[asked + members : 2 * asked + members + 2]
        key_blocks, values_t, query_t, mixed, peak, total, held = refs[2 * asked + members + 2 :]
        step = pl.program_id(0)
        ctx = lax.axis_index("ctx")
        live = spans_ref[0, 0] + spans_ref[0, 1]
        block = ctx ^ flips[which[0]]
        for m in range(1, asked):
            block = jnp.where(step == m, ctx ^ flips[which[m]], block)

        @pl.when(step == 0)
        def _():
            rest = [rest_ref.at[m] for m in range(members - 1)]
            for m, source in enumerate((*own_refs, first_ref, *rest)):
                there = ctx ^ flips[m] if m < members else ctx ^ 1 ^ flips[m - members]
                key_blocks[there] = source[0]
                values_t[there] = source[1].T

        @pl.when(block * rows >= live)
        def _():
            for m in range(asked):

                @pl.when(step == m)
                def _():
                    o_refs[m][...] = jnp.zeros_like(o_refs[m])

        @pl.when(block * rows < live)
        def _():
            for m in range(asked):

                @pl.when(step == m)
                def _():
                    for h in range(heads):
                        query_t[:, h * rows : (h + 1) * rows] = q_refs[m][h].T

            mixed[...] = jnp.zeros_like(mixed)
            peak[...] = jnp.full_like(peak, far_below)
            total[...] = jnp.zeros_like(total)

            def scores(j, part):
                return jnp.dot(key_blocks[j], query_t[:, part], preferred_element_type=jnp.float32)

            def fold(s, j, part):
                old = peak[:, part]
                new = jnp.maximum(old, jnp.max(s, axis=0, keepdims=True))
                weights = jnp.exp2((s - new) * log2_scale)
                factor = jnp.exp2((old - new) * log2_scale)
                total[:, part] = total[:, part] * factor + jnp.sum(weights, axis=0, keepdims=True)
                mixed[:, part] = mixed[:, part] * factor + jnp.dot(
                    values_t[j], weights.astype(jnp.bfloat16), preferred_element_type=jnp.float32
                )
                peak[:, part] = new

            parts = [slice(a, a + part_size) for a in range(0, columns, part_size)]

            def earlier(slot, j):
                for part in parts:
                    s = held[slot, :, part]
                    held[1 - slot, :, part] = scores(j + 1, part)
                    fold(s, j, part)

            def diagonal(slot):
                for part in parts:
                    key_row = lax.broadcasted_iota(jnp.int32, (rows, part_size), 0)
                    key_pos = lax.rem(key_row, rows // stripes) * stripes + key_row // (rows // stripes)
                    query_pos = lax.broadcasted_iota(jnp.int32, (rows, part_size), 1) + part.start
                    allowed = key_pos <= lax.rem(query_pos, rows)
                    fold(jnp.where(allowed, held[slot, :, part], far_below), block, part)

            for part in parts:
                held[0, :, part] = scores(0, part)

            def two(t, carry):
                earlier(0, 2 * t)
                earlier(1, 2 * t + 1)
                return carry

            lax.fori_loop(0, block // 2, two, 0)

            @pl.when(lax.rem(block, 2) == 1)
            def _():
                earlier(0, block - 1)
                diagonal(1)

            @pl.when(lax.rem(block, 2) == 0)
            def _():
                diagonal(0)

            position = block * rows + lax.broadcasted_iota(jnp.int32, (rows, 1), 0)
            for h in range(heads):
                part = slice(h * rows, (h + 1) * rows)
                mixture = (mixed[:, part] / total[:, part]).T
                mixture = jnp.where(position < live, mixture, 0.0).astype(jnp.bfloat16)
                for m in range(asked):

                    @pl.when(step == m)
                    def _():
                        o_refs[m][h] = mixture

    arrays = (*queries, *own, other_first, other_rest)
    return pl.pallas_call(
        kernel,
        grid_spec=pltpu.PrefetchScalarGridSpec(
            num_scalar_prefetch=0,
            grid=(asked,),
            in_specs=[pl.BlockSpec(memory_space=pltpu.SMEM)] + [whole(array) for array in arrays],
            out_specs=[whole(query) for query in queries],
            scratch_shapes=[
                pltpu.VMEM((blocks, rows, width), jnp.bfloat16),
                pltpu.VMEM((blocks, width, rows), jnp.bfloat16),
                pltpu.VMEM((width, columns), jnp.bfloat16),
                pltpu.VMEM((width, columns), jnp.float32),
                pltpu.VMEM((1, columns), jnp.float32),
                pltpu.VMEM((1, columns), jnp.float32),
                pltpu.VMEM((2, rows, columns), jnp.float32),
            ],
        ),
        out_shape=[jax.ShapeDtypeStruct(queries[0].shape, jnp.bfloat16)] * asked,
        compiler_params=pltpu.CompilerParams(
            dimension_semantics=("arbitrary",), vmem_limit_bytes=30 * 1024 * 1024
        ),
        cost_estimate=pl.CostEstimate(
            flops=4 * asked * members * heads * rows * rows * width,
            bytes_accessed=4 * rows * width * (asked * heads + 2 * members),
            transcendentals=asked * members * rows * rows * heads,
        ),
    )(spans, *arrays)


def take_blocks(array, order):
    def kernel(order_ref, in_ref, out_ref):
        for i in range(array.shape[0]):
            out_ref[i] = in_ref[order_ref[i]]

    return pl.pallas_call(
        kernel,
        in_specs=[pl.BlockSpec(memory_space=pltpu.SMEM), whole(array)],
        out_specs=whole(array),
        out_shape=jax.ShapeDtypeStruct(array.shape, array.dtype),
        compiler_params=small(8),
    )(order, array)


def swap(array, axis):
    return lax.all_to_all(array, axis, split_axis=0, concat_axis=0, tiled=True)


def send(array, flip):
    return lax.ppermute(array, "ctx", route(flip))


def device_step(queries, keys, values, spans, partner):
    rows, _, width = queries.shape
    kv_heads = keys.shape[1]
    blocks = lax.axis_size("ctx")
    slots = lax.axis_size("prompt")
    stripes = slots // kv_heads

    by_slot = (rows // stripes, slots, width)
    *kv_out, slot_rows = pack_kv(keys.reshape(by_slot), values.reshape(by_slot), spans, kv_heads)
    own = [kv_out[0]] + [send(kv_out[k], flips[k]) for k in (1, 2, 3)]
    other_first = send(kv_out[0], 1)
    queries, slot_rows, *kv_out = lax.optimization_barrier((queries, slot_rows, *kv_out))
    q_out = pack_queries(queries)
    q_own = [q_out[0]] + [send(q_out[k], flips[k]) for k in (1, 2, 3)]
    other_rest = send(jnp.stack(own[1:]), 1)

    by_prompt = swap(slot_rows, "prompt")
    by_row = take_blocks(by_prompt, partner)
    cache = swap(by_row, "ctx")
    held_rows = slots // blocks
    cache = cache.reshape(blocks, held_rows, 2, rows // stripes, width).transpose(1, 2, 0, 3, 4)

    done = [None] * 4
    for which in ((1, 2), (3, 0)):
        asked = [q_own[k] for k in which]
        for k, result in zip(which, attend(which, asked, own, other_first, other_rest, spans, stripes)):
            done[k] = result
    back = [done[0]] + [send(done[k], flips[k]) for k in (1, 2, 3)]
    return join_heads(back), cache[:, :, None]


def solution(mesh):
    placed = P(("prompt", "ctx"), None, None)
    return jax.shard_map(
        device_step,
        mesh=mesh,
        in_specs=(placed, placed, placed, P("prompt", None), P()),
        out_specs=(placed, P("ctx", None, "prompt", None, None, None)),
        check_vma=False,
    )
```

```python
import math

import jax
import jax.numpy as jnp
from jax import lax
from jax.experimental import pallas as pl
from jax.experimental.pallas import tpu as pltpu
from jax.sharding import PartitionSpec as P

far_below = -1e30


flips = (0, 3, 4, 7)


def route(flip):
    return [(c, c ^ flip) for c in range(8)]


def small(limit):
    return pltpu.CompilerParams(vmem_limit_bytes=limit * 1024 * 1024)


def whole(array):
    return pl.BlockSpec(array.shape, lambda *_: (0,) * len(array.shape))


def pack_kv(keys, values, spans, kv_heads):
    short, slots, width = keys.shape
    stripes = slots // kv_heads
    rows = short * stripes

    def kernel(spans_ref, k_ref, v_ref, *refs):
        outs, slot_ref = refs[:4], refs[4]
        span, k_in, v_in, turned, sems = refs[5:]
        copies = [
            pltpu.make_async_copy(source, target, sems.at[i])
            for i, (source, target) in enumerate(((k_ref, k_in), (v_ref, v_in), (spans_ref, span)))
        ]
        for copy in copies:
            copy.start()
        ctx = lax.axis_index("ctx")
        group, first = ctx // 2, ctx * rows
        for t, ref in enumerate((k_in, v_in)):
            copies[t].wait()
            turned[t] = jnp.swapaxes(ref[...], 0, 1)
        copies[2].wait()
        live = span[0, 0] + span[0, 1]
        for k in range(4):
            for t in range(2):
                for stripe in range(stripes):
                    outs[k][t, stripe * short : (stripe + 1) * short, :] = turned[
                        t, stripe * kv_heads + (group ^ k)
                    ]
        for slot in range(slots):
            position = (
                first + lax.broadcasted_iota(jnp.int32, (short, 1), 0) * stripes + slot // kv_heads
            )
            for t in range(2):
                slot_ref[slot, t] = jnp.where(
                    position < live, turned[t, slot].astype(jnp.float32), 0.0
                ).astype(jnp.bfloat16)

    piece = jax.ShapeDtypeStruct((2, rows, width), jnp.bfloat16)
    out_shape = [piece] * 4 + [jax.ShapeDtypeStruct((slots, 2, short, width), jnp.bfloat16)]
    return pl.pallas_call(
        kernel,
        in_specs=[pl.BlockSpec(memory_space=pltpu.HBM)] * 3,
        out_specs=[whole(out) for out in out_shape],
        out_shape=out_shape,
        scratch_shapes=[
            pltpu.SMEM(spans.shape, jnp.int32),
            pltpu.VMEM(keys.shape, jnp.bfloat16),
            pltpu.VMEM(keys.shape, jnp.bfloat16),
            pltpu.VMEM((2, slots, short, width), jnp.bfloat16),
            pltpu.SemaphoreType.DMA((3,)),
        ],
        compiler_params=small(62),
    )(spans, keys, values)


def pack_queries(queries):
    rows, head_count, width = queries.shape
    heads = head_count // 4

    def kernel(q_ref, *refs):
        outs, turned = refs[:4], refs[4]
        group = lax.axis_index("ctx") // 2
        turned[...] = jnp.swapaxes(q_ref[...], 0, 1)
        for k in range(4):
            outs[k][...] = turned[pl.ds((group ^ k) * heads, heads)]

    piece = jax.ShapeDtypeStruct((heads, rows, width), jnp.bfloat16)
    return pl.pallas_call(
        kernel,
        in_specs=[whole(queries)],
        out_specs=[whole(piece)] * 4,
        out_shape=[piece] * 4,
        scratch_shapes=[pltpu.VMEM((head_count, rows, width), jnp.bfloat16)],
        compiler_params=small(16),
    )(queries)


def join_heads(pieces):
    heads, rows, width = pieces[0].shape

    def kernel(*refs):
        ins, out, gathered = refs[:4], refs[4], refs[5]
        group = lax.axis_index("ctx") // 2
        for k in range(4):
            gathered[pl.ds((group ^ k) * heads, heads)] = ins[k][...]
        out[...] = jnp.swapaxes(gathered[...], 0, 1)

    out_shape = jax.ShapeDtypeStruct((rows, 4 * heads, width), jnp.bfloat16)
    return pl.pallas_call(
        kernel,
        in_specs=[whole(piece) for piece in pieces],
        out_specs=whole(out_shape),
        out_shape=out_shape,
        scratch_shapes=[pltpu.VMEM((4 * heads, rows, width), jnp.bfloat16)],
        compiler_params=small(16),
    )(*pieces)


def attend(which, queries, own, other_first, other_rest, spans, stripes):
    asked = len(which)
    members = len(own)
    heads, rows, width = queries[0].shape
    columns = heads * rows
    part_size = min(columns, 512)
    blocks = 2 * members
    log2_scale = 1.4426950408889634 / math.sqrt(width)

    def kernel(spans_ref, *refs):
        q_refs, own_refs = refs[:asked], refs[asked : asked + members]
        first_ref, rest_ref, *o_refs = refs[asked + members : 2 * asked + members + 2]
        key_blocks, values_t, query_t, mixed, peak, held = refs[2 * asked + members + 2 :]
        step = pl.program_id(0)
        ctx = lax.axis_index("ctx")
        live = spans_ref[0, 0] + spans_ref[0, 1]
        block = ctx ^ flips[which[0]]
        for m in range(1, asked):
            block = jnp.where(step == m, ctx ^ flips[which[m]], block)

        @pl.when(step == 0)
        def _():
            rest = [rest_ref.at[m] for m in range(members - 1)]
            for m, source in enumerate((*own_refs, first_ref, *rest)):
                there = ctx ^ flips[m] if m < members else ctx ^ 1 ^ flips[m - members]
                key_blocks[there] = source[0]
                values_t[there, :width] = source[1].T
            values_t[:, width:] = jnp.ones_like(values_t[:, width:])

        @pl.when(block * rows >= live)
        def _():
            for m in range(asked):

                @pl.when(step == m)
                def _():
                    o_refs[m][...] = jnp.zeros_like(o_refs[m])

        @pl.when(block * rows < live)
        def _():
            for m in range(asked):

                @pl.when(step == m)
                def _():
                    for h in range(heads):
                        query_t[:, h * rows : (h + 1) * rows] = q_refs[m][h].T

            mixed[...] = jnp.zeros_like(mixed)
            peak[...] = jnp.full_like(peak, far_below)

            def scores(j, part):
                return jnp.dot(key_blocks[j], query_t[:, part], preferred_element_type=jnp.float32)

            def fold(s, j, part):
                old = peak[:, part]
                new = jnp.maximum(old, jnp.max(s, axis=0, keepdims=True))
                weights = jnp.exp2((s - new) * log2_scale)
                factor = jnp.exp2((old - new) * log2_scale)
                mixed[:, part] = mixed[:, part] * factor + jnp.dot(
                    values_t[j], weights.astype(jnp.bfloat16), preferred_element_type=jnp.float32
                )
                peak[:, part] = new

            parts = [slice(a, a + part_size) for a in range(0, columns, part_size)]

            def earlier(slot, j):
                for part in parts:
                    s = held[slot, :, part]
                    held[1 - slot, :, part] = scores(j + 1, part)
                    fold(s, j, part)

            def diagonal(slot):
                for part in parts:
                    key_row = lax.broadcasted_iota(jnp.int32, (rows, part_size), 0)
                    key_pos = lax.rem(key_row, rows // stripes) * stripes + key_row // (rows // stripes)
                    query_pos = lax.broadcasted_iota(jnp.int32, (rows, part_size), 1) + part.start
                    allowed = key_pos <= lax.rem(query_pos, rows)
                    fold(jnp.where(allowed, held[slot, :, part], far_below), block, part)

            for part in parts:
                held[0, :, part] = scores(0, part)

            def two(t, carry):
                earlier(0, 2 * t)
                earlier(1, 2 * t + 1)
                return carry

            lax.fori_loop(0, block // 2, two, 0)

            @pl.when(lax.rem(block, 2) == 1)
            def _():
                earlier(0, block - 1)
                diagonal(1)

            @pl.when(lax.rem(block, 2) == 0)
            def _():
                diagonal(0)

            position = block * rows + lax.broadcasted_iota(jnp.int32, (rows, 1), 0)
            for h in range(heads):
                part = slice(h * rows, (h + 1) * rows)
                mixture = (mixed[:width, part] / mixed[width : width + 1, part]).T
                mixture = jnp.where(position < live, mixture, 0.0).astype(jnp.bfloat16)
                for m in range(asked):

                    @pl.when(step == m)
                    def _():
                        o_refs[m][h] = mixture

    arrays = (*queries, *own, other_first, other_rest)
    return pl.pallas_call(
        kernel,
        grid_spec=pltpu.PrefetchScalarGridSpec(
            num_scalar_prefetch=0,
            grid=(asked,),
            in_specs=[pl.BlockSpec(memory_space=pltpu.SMEM)] + [whole(array) for array in arrays],
            out_specs=[whole(query) for query in queries],
            scratch_shapes=[
                pltpu.VMEM((blocks, rows, width), jnp.bfloat16),
                pltpu.VMEM((blocks, width + 16, rows), jnp.bfloat16),
                pltpu.VMEM((width, columns), jnp.bfloat16),
                pltpu.VMEM((width + 16, columns), jnp.float32),
                pltpu.VMEM((1, columns), jnp.float32),
                pltpu.VMEM((2, rows, columns), jnp.float32),
            ],
        ),
        out_shape=[jax.ShapeDtypeStruct(queries[0].shape, jnp.bfloat16)] * asked,
        compiler_params=pltpu.CompilerParams(
            dimension_semantics=("arbitrary",), vmem_limit_bytes=30 * 1024 * 1024
        ),
        cost_estimate=pl.CostEstimate(
            flops=4 * asked * members * heads * rows * rows * width,
            bytes_accessed=4 * rows * width * (asked * heads + 2 * members),
            transcendentals=asked * members * rows * rows * heads,
        ),
    )(spans, *arrays)


def take_blocks(array, order):
    def kernel(order_ref, in_ref, out_ref):
        for i in range(array.shape[0]):
            out_ref[i] = in_ref[order_ref[i]]

    return pl.pallas_call(
        kernel,
        in_specs=[pl.BlockSpec(memory_space=pltpu.SMEM), whole(array)],
        out_specs=whole(array),
        out_shape=jax.ShapeDtypeStruct(array.shape, array.dtype),
        compiler_params=small(8),
    )(order, array)


def swap(array, axis):
    return lax.all_to_all(array, axis, split_axis=0, concat_axis=0, tiled=True)


def send(array, flip):
    return lax.ppermute(array, "ctx", route(flip))


def device_step(queries, keys, values, spans, partner):
    rows, _, width = queries.shape
    kv_heads = keys.shape[1]
    blocks = lax.axis_size("ctx")
    slots = lax.axis_size("prompt")
    stripes = slots // kv_heads

    by_slot = (rows // stripes, slots, width)
    *kv_out, slot_rows = pack_kv(keys.reshape(by_slot), values.reshape(by_slot), spans, kv_heads)
    own = [kv_out[0]] + [send(kv_out[k], flips[k]) for k in (1, 2, 3)]
    other_first = send(kv_out[0], 1)
    q_out = pack_queries(queries)
    q_own = [q_out[0]] + [send(q_out[k], flips[k]) for k in (1, 2, 3)]
    other_rest = send(jnp.stack(own[1:]), 1)

    by_prompt = swap(slot_rows, "prompt")
    by_row = take_blocks(by_prompt, partner)
    cache = swap(by_row, "ctx")
    held_rows = slots // blocks
    cache = cache.reshape(blocks, held_rows, 2, rows // stripes, width).transpose(1, 2, 0, 3, 4)

    done = [None] * 4
    for which in ((1, 2), (3, 0)):
        asked = [q_own[k] for k in which]
        for k, result in zip(which, attend(which, asked, own, other_first, other_rest, spans, stripes)):
            done[k] = result
    back = [done[0]] + [send(done[k], flips[k]) for k in (1, 2, 3)]
    return join_heads(back), cache[:, :, None]


def solution(mesh):
    placed = P(("prompt", "ctx"), None, None)
    return jax.shard_map(
        device_step,
        mesh=mesh,
        in_specs=(placed, placed, placed, P("prompt", None), P()),
        out_specs=(placed, P("ctx", None, "prompt", None, None, None)),
        check_vma=False,
    )
```

```python
import math

import jax
import jax.numpy as jnp
from jax import lax
from jax.experimental import pallas as pl
from jax.experimental.pallas import tpu as pltpu
from jax.sharding import PartitionSpec as P

far_below = -1e30


flips = (0, 3, 4, 7)


def route(flip):
    return [(c, c ^ flip) for c in range(8)]


def small(limit):
    return pltpu.CompilerParams(vmem_limit_bytes=limit * 1024 * 1024)


def whole(array):
    return pl.BlockSpec(array.shape, lambda *_: (0,) * len(array.shape))


def pack_kv(keys, values, spans, kv_heads):
    short, slots, width = keys.shape
    stripes = slots // kv_heads
    rows = short * stripes

    def kernel(spans_ref, k_ref, v_ref, *refs):
        outs, slot_ref = refs[:4], refs[4]
        span, k_in, v_in, turned, sems = refs[5:]
        copies = [
            pltpu.make_async_copy(source, target, sems.at[i])
            for i, (source, target) in enumerate(((k_ref, k_in), (v_ref, v_in), (spans_ref, span)))
        ]
        for copy in copies:
            copy.start()
        ctx = lax.axis_index("ctx")
        group, first = ctx // 2, ctx * rows
        for t, ref in enumerate((k_in, v_in)):
            copies[t].wait()
            turned[t] = jnp.swapaxes(ref[...], 0, 1)
        copies[2].wait()
        live = span[0, 0] + span[0, 1]
        for k in range(4):
            for t in range(2):
                for stripe in range(stripes):
                    outs[k][t, stripe * short : (stripe + 1) * short, :] = turned[
                        t, stripe * kv_heads + (group ^ k)
                    ]
        for slot in range(slots):
            position = (
                first + lax.broadcasted_iota(jnp.int32, (short, 1), 0) * stripes + slot // kv_heads
            )
            for t in range(2):
                slot_ref[slot, t] = jnp.where(
                    position < live, turned[t, slot].astype(jnp.float32), 0.0
                ).astype(jnp.bfloat16)

    piece = jax.ShapeDtypeStruct((2, rows, width), jnp.bfloat16)
    out_shape = [piece] * 4 + [jax.ShapeDtypeStruct((slots, 2, short, width), jnp.bfloat16)]
    return pl.pallas_call(
        kernel,
        in_specs=[pl.BlockSpec(memory_space=pltpu.HBM)] * 3,
        out_specs=[whole(out) for out in out_shape],
        out_shape=out_shape,
        scratch_shapes=[
            pltpu.SMEM(spans.shape, jnp.int32),
            pltpu.VMEM(keys.shape, jnp.bfloat16),
            pltpu.VMEM(keys.shape, jnp.bfloat16),
            pltpu.VMEM((2, slots, short, width), jnp.bfloat16),
            pltpu.SemaphoreType.DMA((3,)),
        ],
        compiler_params=small(62),
    )(spans, keys, values)


def pack_queries(queries):
    rows, head_count, width = queries.shape
    heads = head_count // 4

    def kernel(q_ref, *refs):
        outs, turned = refs[:4], refs[4]
        group = lax.axis_index("ctx") // 2
        turned[...] = jnp.swapaxes(q_ref[...], 0, 1)
        for k in range(4):
            outs[k][...] = turned[pl.ds((group ^ k) * heads, heads)]

    piece = jax.ShapeDtypeStruct((heads, rows, width), jnp.bfloat16)
    return pl.pallas_call(
        kernel,
        in_specs=[whole(queries)],
        out_specs=[whole(piece)] * 4,
        out_shape=[piece] * 4,
        scratch_shapes=[pltpu.VMEM((head_count, rows, width), jnp.bfloat16)],
        compiler_params=small(16),
    )(queries)


def join_heads(pieces):
    heads, rows, width = pieces[0].shape

    def kernel(*refs):
        ins, out, gathered = refs[:4], refs[4], refs[5]
        group = lax.axis_index("ctx") // 2
        for k in range(4):
            gathered[pl.ds((group ^ k) * heads, heads)] = ins[k][...]
        out[...] = jnp.swapaxes(gathered[...], 0, 1)

    out_shape = jax.ShapeDtypeStruct((rows, 4 * heads, width), jnp.bfloat16)
    return pl.pallas_call(
        kernel,
        in_specs=[whole(piece) for piece in pieces],
        out_specs=whole(out_shape),
        out_shape=out_shape,
        scratch_shapes=[pltpu.VMEM((4 * heads, rows, width), jnp.bfloat16)],
        compiler_params=small(16),
    )(*pieces)


def attend(which, queries, own, other, spans, stripes):
    asked = len(which)
    members = len(own)
    heads, rows, width = queries[0].shape
    columns = heads * rows
    part_size = min(columns, 512)
    blocks = 2 * members
    log2_scale = 1.4426950408889634 / math.sqrt(width)

    def kernel(spans_ref, *refs):
        q_refs, kv_refs = refs[:asked], refs[asked : asked + blocks]
        o_refs = refs[asked + blocks : 2 * asked + blocks]
        key_blocks, values_t, query_t, mixed, peak, held = refs[2 * asked + blocks :]
        step = pl.program_id(0)
        ctx = lax.axis_index("ctx")
        live = spans_ref[0, 0] + spans_ref[0, 1]
        block = ctx ^ flips[which[0]]
        for m in range(1, asked):
            block = jnp.where(step == m, ctx ^ flips[which[m]], block)

        @pl.when(step == 0)
        def _():
            for m, source in enumerate(kv_refs):
                there = ctx ^ flips[m] if m < members else ctx ^ 1 ^ flips[m - members]
                key_blocks[there] = source[0]
                values_t[there, :width] = source[1].T
            values_t[:, width:] = jnp.ones_like(values_t[:, width:])

        @pl.when(block * rows >= live)
        def _():
            for m in range(asked):

                @pl.when(step == m)
                def _():
                    o_refs[m][...] = jnp.zeros_like(o_refs[m])

        @pl.when(block * rows < live)
        def _():
            for m in range(asked):

                @pl.when(step == m)
                def _():
                    for h in range(heads):
                        query_t[:, h * rows : (h + 1) * rows] = q_refs[m][h].T

            mixed[...] = jnp.zeros_like(mixed)
            peak[...] = jnp.full_like(peak, far_below)

            def scores(j, part):
                return jnp.dot(key_blocks[j], query_t[:, part], preferred_element_type=jnp.float32)

            def fold(s, j, part):
                old = peak[:, part]
                new = jnp.maximum(old, jnp.max(s, axis=0, keepdims=True))
                weights = jnp.exp2((s - new) * log2_scale)
                factor = jnp.exp2((old - new) * log2_scale)
                mixed[:, part] = mixed[:, part] * factor + jnp.dot(
                    values_t[j], weights.astype(jnp.bfloat16), preferred_element_type=jnp.float32
                )
                peak[:, part] = new

            parts = [slice(a, a + part_size) for a in range(0, columns, part_size)]

            def earlier(slot, j):
                for part in parts:
                    s = held[slot, :, part]
                    held[1 - slot, :, part] = scores(j + 1, part)
                    fold(s, j, part)

            def diagonal(slot):
                for part in parts:
                    key_row = lax.broadcasted_iota(jnp.int32, (rows, part_size), 0)
                    key_pos = lax.rem(key_row, rows // stripes) * stripes + key_row // (rows // stripes)
                    query_pos = lax.broadcasted_iota(jnp.int32, (rows, part_size), 1) + part.start
                    allowed = key_pos <= lax.rem(query_pos, rows)
                    fold(jnp.where(allowed, held[slot, :, part], far_below), block, part)

            for part in parts:
                held[0, :, part] = scores(0, part)

            def two(t, carry):
                earlier(0, 2 * t)
                earlier(1, 2 * t + 1)
                return carry

            lax.fori_loop(0, block // 2, two, 0)

            @pl.when(lax.rem(block, 2) == 1)
            def _():
                earlier(0, block - 1)
                diagonal(1)

            @pl.when(lax.rem(block, 2) == 0)
            def _():
                diagonal(0)

            position = block * rows + lax.broadcasted_iota(jnp.int32, (rows, 1), 0)
            for h in range(heads):
                part = slice(h * rows, (h + 1) * rows)
                mixture = (mixed[:width, part] / mixed[width : width + 1, part]).T
                mixture = jnp.where(position < live, mixture, 0.0).astype(jnp.bfloat16)
                for m in range(asked):

                    @pl.when(step == m)
                    def _():
                        o_refs[m][h] = mixture

    arrays = (*queries, *own, *other)
    return pl.pallas_call(
        kernel,
        grid_spec=pltpu.PrefetchScalarGridSpec(
            num_scalar_prefetch=0,
            grid=(asked,),
            in_specs=[pl.BlockSpec(memory_space=pltpu.SMEM)] + [whole(array) for array in arrays],
            out_specs=[whole(query) for query in queries],
            scratch_shapes=[
                pltpu.VMEM((blocks, rows, width), jnp.bfloat16),
                pltpu.VMEM((blocks, width + 16, rows), jnp.bfloat16),
                pltpu.VMEM((width, columns), jnp.bfloat16),
                pltpu.VMEM((width + 16, columns), jnp.float32),
                pltpu.VMEM((1, columns), jnp.float32),
                pltpu.VMEM((2, rows, columns), jnp.float32),
            ],
        ),
        out_shape=[jax.ShapeDtypeStruct(queries[0].shape, jnp.bfloat16)] * asked,
        compiler_params=pltpu.CompilerParams(
            dimension_semantics=("arbitrary",), vmem_limit_bytes=30 * 1024 * 1024
        ),
        cost_estimate=pl.CostEstimate(
            flops=4 * asked * members * heads * rows * rows * width,
            bytes_accessed=4 * rows * width * (asked * heads + 2 * members),
            transcendentals=asked * members * rows * rows * heads,
        ),
    )(spans, *arrays)


def take_blocks(array, order):
    def kernel(order_ref, in_ref, out_ref):
        for i in range(array.shape[0]):
            out_ref[i] = in_ref[order_ref[i]]

    return pl.pallas_call(
        kernel,
        in_specs=[pl.BlockSpec(memory_space=pltpu.SMEM), whole(array)],
        out_specs=whole(array),
        out_shape=jax.ShapeDtypeStruct(array.shape, array.dtype),
        compiler_params=small(8),
    )(order, array)


def place_rows(cache, held_rows):
    count, two, short, width = cache.shape
    blocks = count // held_rows
    out_shape = jax.ShapeDtypeStruct((held_rows, two, 1, blocks, short, width), cache.dtype)

    def kernel(in_ref, out_ref):
        for i in range(count):
            for t in range(two):
                out_ref[i % held_rows, t, 0, i // held_rows] = in_ref[i, t]

    return pl.pallas_call(
        kernel,
        in_specs=[whole(cache)],
        out_specs=whole(out_shape),
        out_shape=out_shape,
        compiler_params=small(8),
    )(cache)


def swap(array, axis):
    return lax.all_to_all(array, axis, split_axis=0, concat_axis=0, tiled=True)


def send(array, flip):
    return lax.ppermute(array, "ctx", route(flip))


def device_step(queries, keys, values, spans, partner):
    rows, _, width = queries.shape
    kv_heads = keys.shape[1]
    blocks = lax.axis_size("ctx")
    slots = lax.axis_size("prompt")
    stripes = slots // kv_heads

    by_slot = (rows // stripes, slots, width)
    *kv_out, slot_rows = pack_kv(keys.reshape(by_slot), values.reshape(by_slot), spans, kv_heads)
    own = [kv_out[0]] + [send(kv_out[k], flips[k]) for k in (1, 2, 3)]
    other_first = send(kv_out[0], 1)
    q_out = pack_queries(queries)
    q_own = [q_out[0]] + [send(q_out[k], flips[k]) for k in (1, 2, 3)]
    other = [other_first] + [send(own[k], 1) for k in (1, 2, 3)]

    by_prompt = swap(slot_rows, "prompt")
    by_row = take_blocks(by_prompt, partner)
    cache = swap(by_row, "ctx")
    cache = place_rows(cache, slots // blocks)

    done = [None] * 4
    for which in ((1, 2), (3, 0)):
        asked = [q_own[k] for k in which]
        for k, result in zip(which, attend(which, asked, own, other, spans, stripes)):
            done[k] = result
    back = [done[0]] + [send(done[k], flips[k]) for k in (1, 2, 3)]
    return join_heads(back), cache


def solution(mesh):
    placed = P(("prompt", "ctx"), None, None)
    return jax.shard_map(
        device_step,
        mesh=mesh,
        in_specs=(placed, placed, placed, P("prompt", None), P()),
        out_specs=(placed, P("ctx", None, "prompt", None, None, None)),
        check_vma=False,
    )
```

```python
import math

import jax
import jax.numpy as jnp
from jax import lax
from jax.experimental import pallas as pl
from jax.experimental.pallas import tpu as pltpu
from jax.sharding import PartitionSpec as P

far_below = -1e30


flips = (0, 3, 4, 7)


def route(flip):
    return [(c, c ^ flip) for c in range(8)]


def small(limit):
    return pltpu.CompilerParams(vmem_limit_bytes=limit * 1024 * 1024)


def whole(array):
    return pl.BlockSpec(array.shape, lambda *_: (0,) * len(array.shape))


def pack_kv(keys, values, spans, kv_heads):
    short, slots, width = keys.shape
    stripes = slots // kv_heads
    rows = short * stripes

    def kernel(spans_ref, k_ref, v_ref, *refs):
        outs, slot_ref = refs[:4], refs[4]
        span, k_in, v_in, turned, sems = refs[5:]
        copies = [
            pltpu.make_async_copy(source, target, sems.at[i])
            for i, (source, target) in enumerate(((k_ref, k_in), (v_ref, v_in), (spans_ref, span)))
        ]
        for copy in copies:
            copy.start()
        ctx = lax.axis_index("ctx")
        group, first = ctx // 2, ctx * rows
        for t, ref in enumerate((k_in, v_in)):
            copies[t].wait()
            turned[t] = jnp.swapaxes(ref[...], 0, 1)
        copies[2].wait()
        live = span[0, 0] + span[0, 1]
        for k in range(4):
            for t in range(2):
                for stripe in range(stripes):
                    outs[k][t, stripe * short : (stripe + 1) * short, :] = turned[
                        t, stripe * kv_heads + (group ^ k)
                    ]
        for slot in range(slots):
            position = (
                first + lax.broadcasted_iota(jnp.int32, (short, 1), 0) * stripes + slot // kv_heads
            )
            for t in range(2):
                slot_ref[slot, t] = jnp.where(
                    position < live, turned[t, slot].astype(jnp.float32), 0.0
                ).astype(jnp.bfloat16)

    piece = jax.ShapeDtypeStruct((2, rows, width), jnp.bfloat16)
    out_shape = [piece] * 4 + [jax.ShapeDtypeStruct((slots, 2, short, width), jnp.bfloat16)]
    return pl.pallas_call(
        kernel,
        in_specs=[pl.BlockSpec(memory_space=pltpu.HBM)] * 3,
        out_specs=[whole(out) for out in out_shape],
        out_shape=out_shape,
        scratch_shapes=[
            pltpu.SMEM(spans.shape, jnp.int32),
            pltpu.VMEM(keys.shape, jnp.bfloat16),
            pltpu.VMEM(keys.shape, jnp.bfloat16),
            pltpu.VMEM((2, slots, short, width), jnp.bfloat16),
            pltpu.SemaphoreType.DMA((3,)),
        ],
        compiler_params=small(62),
    )(spans, keys, values)


def pack_queries(queries):
    rows, head_count, width = queries.shape
    heads = head_count // 4

    def kernel(q_ref, *refs):
        outs, turned = refs[:4], refs[4]
        group = lax.axis_index("ctx") // 2
        turned[...] = jnp.swapaxes(q_ref[...], 0, 1)
        for k in range(4):
            outs[k][...] = turned[pl.ds((group ^ k) * heads, heads)]

    piece = jax.ShapeDtypeStruct((heads, rows, width), jnp.bfloat16)
    return pl.pallas_call(
        kernel,
        in_specs=[whole(queries)],
        out_specs=[whole(piece)] * 4,
        out_shape=[piece] * 4,
        scratch_shapes=[pltpu.VMEM((head_count, rows, width), jnp.bfloat16)],
        compiler_params=small(16),
    )(queries)


def join_heads(pieces):
    heads, rows, width = pieces[0].shape

    def kernel(*refs):
        ins, out, gathered = refs[:4], refs[4], refs[5]
        group = lax.axis_index("ctx") // 2
        for k in range(4):
            gathered[pl.ds((group ^ k) * heads, heads)] = ins[k][...]
        out[...] = jnp.swapaxes(gathered[...], 0, 1)

    out_shape = jax.ShapeDtypeStruct((rows, 4 * heads, width), jnp.bfloat16)
    return pl.pallas_call(
        kernel,
        in_specs=[whole(piece) for piece in pieces],
        out_specs=whole(out_shape),
        out_shape=out_shape,
        scratch_shapes=[pltpu.VMEM((4 * heads, rows, width), jnp.bfloat16)],
        compiler_params=small(16),
    )(*pieces)


def attend(which, queries, own, other, spans, stripes):
    asked = len(which)
    members = len(own)
    heads, rows, width = queries[0].shape
    columns = heads * rows
    part_size = min(columns, 512)
    blocks = 2 * members
    log2_scale = 1.4426950408889634 / math.sqrt(width)

    def kernel(spans_ref, *refs):
        q_refs, kv_refs = refs[:asked], refs[asked : asked + blocks]
        o_refs = refs[asked + blocks : 2 * asked + blocks]
        scratch = refs[2 * asked + blocks :]
        q_in, values_in, key_blocks, values_t, query_t, mixed, peak, held, o_out, q_sem, k_sem, v_sem, o_sem = scratch
        step = pl.program_id(0)
        ctx = lax.axis_index("ctx")
        live = spans_ref[0, 0] + spans_ref[0, 1]
        block = ctx ^ flips[which[0]]
        for m in range(1, asked):
            block = jnp.where(step == m, ctx ^ flips[which[m]], block)
        theres = [ctx ^ flip for flip in flips] + [ctx ^ 1 ^ flip for flip in flips]
        q_copies = [
            pltpu.make_async_copy(q_refs[m], q_in.at[m], q_sem.at[m]) for m in range(asked)
        ]
        k_copies = [
            pltpu.make_async_copy(kv_refs[m].at[0], key_blocks.at[theres[m]], k_sem.at[m])
            for m in range(blocks)
        ]
        v_copies = [
            pltpu.make_async_copy(kv_refs[m].at[1], values_in.at[m], v_sem.at[m])
            for m in range(blocks)
        ]
        o_copies = [
            pltpu.make_async_copy(o_out.at[m], o_refs[m], o_sem.at[m]) for m in range(asked)
        ]

        @pl.when(step == 0)
        def _():
            for copy in (*v_copies, *q_copies, *k_copies):
                copy.start()
            values_t[:, width:] = jnp.ones_like(values_t[:, width:])
            for m in range(blocks):
                v_copies[m].wait()
                values_t[theres[m], :width] = values_in[m].T
            for copy in (*q_copies, *k_copies):
                copy.wait()

        @pl.when(block * rows >= live)
        def _():
            o_out[step] = jnp.zeros(o_out.shape[1:], o_out.dtype)

        @pl.when(block * rows < live)
        def _():
            for h in range(heads):
                query_t[:, h * rows : (h + 1) * rows] = q_in[step, h].T
            mixed[...] = jnp.zeros_like(mixed)
            peak[...] = jnp.full_like(peak, far_below)

            def scores(j, part):
                return jnp.dot(key_blocks[j], query_t[:, part], preferred_element_type=jnp.float32)

            def fold(s, j, part):
                old = peak[:, part]
                new = jnp.maximum(old, jnp.max(s, axis=0, keepdims=True))
                weights = jnp.exp2((s - new) * log2_scale)
                factor = jnp.exp2((old - new) * log2_scale)
                mixed[:, part] = mixed[:, part] * factor + jnp.dot(
                    values_t[j], weights.astype(jnp.bfloat16), preferred_element_type=jnp.float32
                )
                peak[:, part] = new

            parts = [slice(a, a + part_size) for a in range(0, columns, part_size)]

            def earlier(slot, j):
                for part in parts:
                    s = held[slot, :, part]
                    held[1 - slot, :, part] = scores(j + 1, part)
                    fold(s, j, part)

            def diagonal(slot):
                for part in parts:
                    key_row = lax.broadcasted_iota(jnp.int32, (rows, part_size), 0)
                    key_pos = lax.rem(key_row, rows // stripes) * stripes + key_row // (rows // stripes)
                    query_pos = lax.broadcasted_iota(jnp.int32, (rows, part_size), 1) + part.start
                    allowed = key_pos <= lax.rem(query_pos, rows)
                    fold(jnp.where(allowed, held[slot, :, part], far_below), block, part)

            for part in parts:
                held[0, :, part] = scores(0, part)

            def two(t, carry):
                earlier(0, 2 * t)
                earlier(1, 2 * t + 1)
                return carry

            lax.fori_loop(0, block // 2, two, 0)

            @pl.when(lax.rem(block, 2) == 1)
            def _():
                earlier(0, block - 1)
                diagonal(1)

            @pl.when(lax.rem(block, 2) == 0)
            def _():
                diagonal(0)

            position = block * rows + lax.broadcasted_iota(jnp.int32, (rows, 1), 0)
            for h in range(heads):
                part = slice(h * rows, (h + 1) * rows)
                mixture = (mixed[:width, part] / mixed[width : width + 1, part]).T
                o_out[step, h] = jnp.where(position < live, mixture, 0.0).astype(jnp.bfloat16)

        for m in range(asked):

            @pl.when(step == m)
            def _():
                o_copies[m].start()

        @pl.when(step == asked - 1)
        def _():
            for copy in o_copies:
                copy.wait()

    arrays = (*queries, *own, *other)
    return pl.pallas_call(
        kernel,
        grid_spec=pltpu.PrefetchScalarGridSpec(
            num_scalar_prefetch=0,
            grid=(asked,),
            in_specs=[pl.BlockSpec(memory_space=pltpu.SMEM)]
            + [pl.BlockSpec(memory_space=pl.ANY)] * len(arrays),
            out_specs=[pl.BlockSpec(memory_space=pl.ANY)] * asked,
            scratch_shapes=[
                pltpu.VMEM((asked, heads, rows, width), jnp.bfloat16),
                pltpu.VMEM((blocks, rows, width), jnp.bfloat16),
                pltpu.VMEM((blocks, rows, width), jnp.bfloat16),
                pltpu.VMEM((blocks, width + 16, rows), jnp.bfloat16),
                pltpu.VMEM((width, columns), jnp.bfloat16),
                pltpu.VMEM((width + 16, columns), jnp.float32),
                pltpu.VMEM((1, columns), jnp.float32),
                pltpu.VMEM((2, rows, columns), jnp.float32),
                pltpu.VMEM((asked, heads, rows, width), jnp.bfloat16),
                pltpu.SemaphoreType.DMA((asked,)),
                pltpu.SemaphoreType.DMA((blocks,)),
                pltpu.SemaphoreType.DMA((blocks,)),
                pltpu.SemaphoreType.DMA((asked,)),
            ],
        ),
        out_shape=[jax.ShapeDtypeStruct(queries[0].shape, jnp.bfloat16)] * asked,
        compiler_params=pltpu.CompilerParams(
            dimension_semantics=("arbitrary",), vmem_limit_bytes=62 * 1024 * 1024
        ),
        cost_estimate=pl.CostEstimate(
            flops=4 * asked * members * heads * rows * rows * width,
            bytes_accessed=4 * rows * width * (asked * heads + 2 * members),
            transcendentals=asked * members * rows * rows * heads,
        ),
    )(spans, *arrays)


def take_blocks(array, order):
    def kernel(order_ref, in_ref, out_ref):
        for i in range(array.shape[0]):
            out_ref[i] = in_ref[order_ref[i]]

    return pl.pallas_call(
        kernel,
        in_specs=[pl.BlockSpec(memory_space=pltpu.SMEM), whole(array)],
        out_specs=whole(array),
        out_shape=jax.ShapeDtypeStruct(array.shape, array.dtype),
        compiler_params=small(8),
    )(order, array)


def place_rows(cache, held_rows):
    count, two, short, width = cache.shape
    blocks = count // held_rows
    out_shape = jax.ShapeDtypeStruct((held_rows, two, 1, blocks, short, width), cache.dtype)

    def kernel(in_ref, out_ref):
        for i in range(count):
            for t in range(two):
                out_ref[i % held_rows, t, 0, i // held_rows] = in_ref[i, t]

    return pl.pallas_call(
        kernel,
        in_specs=[whole(cache)],
        out_specs=whole(out_shape),
        out_shape=out_shape,
        compiler_params=small(8),
    )(cache)


def swap(array, axis):
    return lax.all_to_all(array, axis, split_axis=0, concat_axis=0, tiled=True)


def send(array, flip):
    return lax.ppermute(array, "ctx", route(flip))


def device_step(queries, keys, values, spans, partner):
    rows, _, width = queries.shape
    kv_heads = keys.shape[1]
    blocks = lax.axis_size("ctx")
    slots = lax.axis_size("prompt")
    stripes = slots // kv_heads

    by_slot = (rows // stripes, slots, width)
    *kv_out, slot_rows = pack_kv(keys.reshape(by_slot), values.reshape(by_slot), spans, kv_heads)
    own = [kv_out[0]] + [send(kv_out[k], flips[k]) for k in (1, 2, 3)]
    other_first = send(kv_out[0], 1)
    q_out = pack_queries(queries)
    q_own = [q_out[0]] + [send(q_out[k], flips[k]) for k in (1, 2, 3)]
    other = [other_first] + [send(own[k], 1) for k in (1, 2, 3)]

    by_prompt = swap(slot_rows, "prompt")
    by_row = take_blocks(by_prompt, partner)
    cache = swap(by_row, "ctx")
    cache = place_rows(cache, slots // blocks)

    done = [None] * 4
    for which in ((1, 2), (3, 0)):
        asked = [q_own[k] for k in which]
        for k, result in zip(which, attend(which, asked, own, other, spans, stripes)):
            done[k] = result
    back = [done[0]] + [send(done[k], flips[k]) for k in (1, 2, 3)]
    return join_heads(back), cache


def solution(mesh):
    placed = P(("prompt", "ctx"), None, None)
    return jax.shard_map(
        device_step,
        mesh=mesh,
        in_specs=(placed, placed, placed, P("prompt", None), P()),
        out_specs=(placed, P("ctx", None, "prompt", None, None, None)),
        check_vma=False,
    )
```

```python
import math

import jax
import jax.numpy as jnp
from jax import lax
from jax.experimental import pallas as pl
from jax.experimental.pallas import tpu as pltpu
from jax.sharding import PartitionSpec as P

far_below = -1e30


flips = (0, 3, 4, 7)


def route(flip):
    return [(c, c ^ flip) for c in range(8)]


def small(limit):
    return pltpu.CompilerParams(vmem_limit_bytes=limit * 1024 * 1024)


def whole(array):
    return pl.BlockSpec(array.shape, lambda *_: (0,) * len(array.shape))


def pack_kv(keys, values, spans, kv_heads):
    short, slots, width = keys.shape
    stripes = slots // kv_heads
    rows = short * stripes
    run = short // 2

    def kernel(spans_ref, k_ref, v_ref, *refs):
        outs, slot_ref = refs[:4], refs[4]
        span, k_in, v_in, turned, sems = refs[5:]
        copies = [
            pltpu.make_async_copy(source, target, sems.at[i])
            for i, (source, target) in enumerate(((k_ref, k_in), (v_ref, v_in), (spans_ref, span)))
        ]
        for copy in copies:
            copy.start()
        ctx = lax.axis_index("ctx")
        group, first = ctx // 2, ctx * rows
        for t, ref in enumerate((k_in, v_in)):
            copies[t].wait()
            turned[t] = jnp.swapaxes(ref[...], 0, 1)
        copies[2].wait()
        live = span[0, 0] + span[0, 1]
        for k in range(4):
            for t in range(2):
                for stripe in range(stripes):
                    slot = stripe * kv_heads + (group ^ k)
                    for half in range(2):
                        at = (half * stripes + stripe) * run
                        outs[k][t, at : at + run, :] = turned[t, slot, half * run : (half + 1) * run]
        for slot in range(slots):
            position = (
                first + lax.broadcasted_iota(jnp.int32, (short, 1), 0) * stripes + slot // kv_heads
            )
            for t in range(2):
                slot_ref[slot, t] = jnp.where(
                    position < live, turned[t, slot].astype(jnp.float32), 0.0
                ).astype(jnp.bfloat16)

    piece = jax.ShapeDtypeStruct((2, rows, width), jnp.bfloat16)
    out_shape = [piece] * 4 + [jax.ShapeDtypeStruct((slots, 2, short, width), jnp.bfloat16)]
    return pl.pallas_call(
        kernel,
        in_specs=[pl.BlockSpec(memory_space=pltpu.HBM)] * 3,
        out_specs=[whole(out) for out in out_shape],
        out_shape=out_shape,
        scratch_shapes=[
            pltpu.SMEM(spans.shape, jnp.int32),
            pltpu.VMEM(keys.shape, jnp.bfloat16),
            pltpu.VMEM(keys.shape, jnp.bfloat16),
            pltpu.VMEM((2, slots, short, width), jnp.bfloat16),
            pltpu.SemaphoreType.DMA((3,)),
        ],
        compiler_params=small(62),
    )(spans, keys, values)


def pack_queries(queries):
    rows, head_count, width = queries.shape
    heads = head_count // 4
    chunk = rows // 4

    def kernel(q_ref, *refs):
        outs, turned = refs[:4], refs[4]
        group = lax.axis_index("ctx") // 2
        turned[...] = jnp.swapaxes(q_ref[...], 0, 1)
        for k in range(4):
            outs[k][...] = turned[pl.ds((group ^ k) * heads, heads)]

    piece = jax.ShapeDtypeStruct((heads, rows, width), jnp.bfloat16)
    return pl.pallas_call(
        kernel,
        grid=(4,),
        in_specs=[pl.BlockSpec((chunk, head_count, width), lambda i: (i, 0, 0))],
        out_specs=[pl.BlockSpec((heads, chunk, width), lambda i: (0, i, 0))] * 4,
        out_shape=[piece] * 4,
        scratch_shapes=[pltpu.VMEM((head_count, chunk, width), jnp.bfloat16)],
        compiler_params=small(62),
    )(queries)


def join_heads(pieces):
    heads, rows, width = pieces[0].shape
    chunk = rows // 4

    def kernel(*refs):
        ins, out, gathered = refs[:4], refs[4], refs[5]
        group = lax.axis_index("ctx") // 2
        for k in range(4):
            gathered[pl.ds((group ^ k) * heads, heads)] = ins[k][...]
        out[...] = jnp.swapaxes(gathered[...], 0, 1)

    return pl.pallas_call(
        kernel,
        grid=(4,),
        in_specs=[pl.BlockSpec((heads, chunk, width), lambda i: (0, i, 0))] * 4,
        out_specs=pl.BlockSpec((chunk, 4 * heads, width), lambda i: (i, 0, 0)),
        out_shape=jax.ShapeDtypeStruct((rows, 4 * heads, width), jnp.bfloat16),
        scratch_shapes=[pltpu.VMEM((4 * heads, chunk, width), jnp.bfloat16)],
        compiler_params=small(16),
    )(*pieces)


def attend(which, queries, own, other, spans, stripes):
    asked = len(which)
    members = len(own)
    heads, rows, width = queries[0].shape
    columns = heads * rows
    part_size = min(columns, 512)
    blocks = 2 * members
    log2_scale = 1.4426950408889634 / math.sqrt(width)

    def kernel(spans_ref, *refs):
        q_refs, kv_refs = refs[:asked], refs[asked : asked + blocks]
        o_refs = refs[asked + blocks : 2 * asked + blocks]
        scratch = refs[2 * asked + blocks :]
        q_in, values_in, key_blocks, values_t, query_t, mixed, peak, held, o_out, q_sem, k_sem, v_sem, o_sem = scratch
        step = pl.program_id(0)
        ctx = lax.axis_index("ctx")
        live = spans_ref[0, 0] + spans_ref[0, 1]
        block = ctx ^ flips[which[0]]
        for m in range(1, asked):
            block = jnp.where(step == m, ctx ^ flips[which[m]], block)
        theres = [ctx ^ flip for flip in flips] + [ctx ^ 1 ^ flip for flip in flips]
        q_copies = [
            pltpu.make_async_copy(q_refs[m], q_in.at[m], q_sem.at[m]) for m in range(asked)
        ]
        k_copies = [
            pltpu.make_async_copy(kv_refs[m].at[0], key_blocks.at[theres[m]], k_sem.at[m])
            for m in range(blocks)
        ]
        v_copies = [
            pltpu.make_async_copy(kv_refs[m].at[1], values_in.at[m], v_sem.at[m])
            for m in range(blocks)
        ]
        o_copies = [
            pltpu.make_async_copy(o_out.at[m], o_refs[m], o_sem.at[m]) for m in range(asked)
        ]

        @pl.when(step == 0)
        def _():
            for copy in (*v_copies, *q_copies, *k_copies):
                copy.start()
            values_t[:, width:] = jnp.ones_like(values_t[:, width:])
            for m in range(blocks):
                v_copies[m].wait()
                values_t[theres[m], :width] = values_in[m].T
            for copy in (*q_copies, *k_copies):
                copy.wait()

        @pl.when(block * rows >= live)
        def _():
            o_out[step] = jnp.zeros(o_out.shape[1:], o_out.dtype)

        @pl.when(block * rows < live)
        def _():
            for h in range(heads):
                query_t[:, h * rows : (h + 1) * rows] = q_in[step, h].T
            mixed[...] = jnp.zeros_like(mixed)
            peak[...] = jnp.full_like(peak, far_below)

            def scores(j, part):
                return jnp.dot(key_blocks[j], query_t[:, part], preferred_element_type=jnp.float32)

            def fold(s, j, part, depth=rows):
                old = peak[:, part]
                new = jnp.maximum(old, jnp.max(s, axis=0, keepdims=True))
                weights = jnp.exp2((s - new) * log2_scale)
                factor = jnp.exp2((old - new) * log2_scale)
                mixed[:, part] = mixed[:, part] * factor + jnp.dot(
                    values_t[j, :, :depth],
                    weights.astype(jnp.bfloat16),
                    preferred_element_type=jnp.float32,
                )
                peak[:, part] = new

            parts = [slice(a, a + part_size) for a in range(0, columns, part_size)]

            def earlier(slot, j):
                for part in parts:
                    s = held[slot, :, part]
                    held[1 - slot, :, part] = scores(j + 1, part)
                    fold(s, j, part)

            def diagonal(slot):
                half, run = rows // 2, rows // stripes // 2
                for a in range(0, columns, half):
                    part = slice(a, a + half)
                    depth = half if a % rows == 0 else rows
                    key_row = lax.broadcasted_iota(jnp.int32, (depth, half), 0)
                    within = lax.rem(key_row, half)
                    key_pos = key_row - within + lax.rem(within, run) * stripes + within // run
                    query_pos = lax.broadcasted_iota(jnp.int32, (depth, half), 1) + a % rows
                    s = jnp.where(key_pos <= query_pos, held[slot, :depth, part], far_below)
                    fold(s, block, part, depth)

            for part in parts:
                held[0, :, part] = scores(0, part)

            def two(t, carry):
                earlier(0, 2 * t)
                earlier(1, 2 * t + 1)
                return carry

            lax.fori_loop(0, block // 2, two, 0)

            @pl.when(lax.rem(block, 2) == 1)
            def _():
                earlier(0, block - 1)
                diagonal(1)

            @pl.when(lax.rem(block, 2) == 0)
            def _():
                diagonal(0)

            position = block * rows + lax.broadcasted_iota(jnp.int32, (rows, 1), 0)
            for h in range(heads):
                part = slice(h * rows, (h + 1) * rows)
                mixture = (mixed[:width, part] / mixed[width : width + 1, part]).T
                o_out[step, h] = jnp.where(position < live, mixture, 0.0).astype(jnp.bfloat16)

        for m in range(asked):

            @pl.when(step == m)
            def _():
                o_copies[m].start()

        @pl.when(step == asked - 1)
        def _():
            for copy in o_copies:
                copy.wait()

    arrays = (*queries, *own, *other)
    return pl.pallas_call(
        kernel,
        grid_spec=pltpu.PrefetchScalarGridSpec(
            num_scalar_prefetch=0,
            grid=(asked,),
            in_specs=[pl.BlockSpec(memory_space=pltpu.SMEM)]
            + [pl.BlockSpec(memory_space=pl.ANY)] * len(arrays),
            out_specs=[pl.BlockSpec(memory_space=pl.ANY)] * asked,
            scratch_shapes=[
                pltpu.VMEM((asked, heads, rows, width), jnp.bfloat16),
                pltpu.VMEM((blocks, rows, width), jnp.bfloat16),
                pltpu.VMEM((blocks, rows, width), jnp.bfloat16),
                pltpu.VMEM((blocks, width + 16, rows), jnp.bfloat16),
                pltpu.VMEM((width, columns), jnp.bfloat16),
                pltpu.VMEM((width + 16, columns), jnp.float32),
                pltpu.VMEM((1, columns), jnp.float32),
                pltpu.VMEM((2, rows, columns), jnp.float32),
                pltpu.VMEM((asked, heads, rows, width), jnp.bfloat16),
                pltpu.SemaphoreType.DMA((asked,)),
                pltpu.SemaphoreType.DMA((blocks,)),
                pltpu.SemaphoreType.DMA((blocks,)),
                pltpu.SemaphoreType.DMA((asked,)),
            ],
        ),
        out_shape=[jax.ShapeDtypeStruct(queries[0].shape, jnp.bfloat16)] * asked,
        compiler_params=pltpu.CompilerParams(
            dimension_semantics=("arbitrary",), vmem_limit_bytes=62 * 1024 * 1024
        ),
        cost_estimate=pl.CostEstimate(
            flops=4 * asked * members * heads * rows * rows * width,
            bytes_accessed=4 * rows * width * (asked * heads + 2 * members),
            transcendentals=asked * members * rows * rows * heads,
        ),
    )(spans, *arrays)


def take_blocks(array, order):
    def kernel(order_ref, in_ref, out_ref):
        for i in range(array.shape[0]):
            out_ref[i] = in_ref[order_ref[i]]

    return pl.pallas_call(
        kernel,
        in_specs=[pl.BlockSpec(memory_space=pltpu.SMEM), whole(array)],
        out_specs=whole(array),
        out_shape=jax.ShapeDtypeStruct(array.shape, array.dtype),
        compiler_params=small(8),
    )(order, array)


def place_rows(cache, held_rows):
    count, two, short, width = cache.shape
    blocks = count // held_rows
    out_shape = jax.ShapeDtypeStruct((held_rows, two, 1, blocks, short, width), cache.dtype)

    def kernel(in_ref, out_ref):
        for i in range(count):
            for t in range(two):
                out_ref[i % held_rows, t, 0, i // held_rows] = in_ref[i, t]

    return pl.pallas_call(
        kernel,
        in_specs=[whole(cache)],
        out_specs=whole(out_shape),
        out_shape=out_shape,
        compiler_params=small(8),
    )(cache)


def swap(array, axis):
    return lax.all_to_all(array, axis, split_axis=0, concat_axis=0, tiled=True)


def send(array, flip):
    return lax.ppermute(array, "ctx", route(flip))


def device_step(queries, keys, values, spans, partner):
    rows, _, width = queries.shape
    kv_heads = keys.shape[1]
    blocks = lax.axis_size("ctx")
    slots = lax.axis_size("prompt")
    stripes = slots // kv_heads

    by_slot = (rows // stripes, slots, width)
    *kv_out, slot_rows = pack_kv(keys.reshape(by_slot), values.reshape(by_slot), spans, kv_heads)
    own = [kv_out[0]] + [send(kv_out[k], flips[k]) for k in (1, 2, 3)]
    other_first = send(kv_out[0], 1)
    q_out = pack_queries(queries)
    q_own = [q_out[0]] + [send(q_out[k], flips[k]) for k in (1, 2, 3)]
    other = [other_first] + [send(own[k], 1) for k in (1, 2, 3)]

    by_prompt = swap(slot_rows, "prompt")
    by_row = take_blocks(by_prompt, partner)
    cache = swap(by_row, "ctx")
    cache = place_rows(cache, slots // blocks)

    done = [None] * 4
    for which in ((1, 2), (3, 0)):
        asked = [q_own[k] for k in which]
        for k, result in zip(which, attend(which, asked, own, other, spans, stripes)):
            done[k] = result
    back = [done[0]] + [send(done[k], flips[k]) for k in (1, 2, 3)]
    return join_heads(back), cache


def solution(mesh):
    placed = P(("prompt", "ctx"), None, None)
    return jax.shard_map(
        device_step,
        mesh=mesh,
        in_specs=(placed, placed, placed, P("prompt", None), P()),
        out_specs=(placed, P("ctx", None, "prompt", None, None, None)),
        check_vma=False,
    )
```

```python
import math

import jax
import jax.numpy as jnp
from jax import lax
from jax.experimental import pallas as pl
from jax.experimental.pallas import tpu as pltpu
from jax.sharding import PartitionSpec as P

far_below = -1e30


flips = (0, 3, 4, 7)


def route(flip):
    return [(c, c ^ flip) for c in range(8)]


def small(limit):
    return pltpu.CompilerParams(vmem_limit_bytes=limit * 1024 * 1024)


def whole(array):
    return pl.BlockSpec(array.shape, lambda *_: (0,) * len(array.shape))


def pack_kv(keys, values, spans, kv_heads):
    short, slots, width = keys.shape
    stripes = slots // kv_heads
    rows = short * stripes
    run = short // 2

    def kernel(spans_ref, k_ref, v_ref, *refs):
        outs, slot_ref = refs[:4], refs[4]
        span, k_in, v_in, turned, sems = refs[5:]
        copies = [
            pltpu.make_async_copy(source, target, sems.at[i])
            for i, (source, target) in enumerate(((k_ref, k_in), (v_ref, v_in), (spans_ref, span)))
        ]
        for copy in copies:
            copy.start()
        ctx = lax.axis_index("ctx")
        group, first = ctx // 2, ctx * rows
        for t, ref in enumerate((k_in, v_in)):
            copies[t].wait()
            turned[t] = jnp.swapaxes(ref[...], 0, 1)
        copies[2].wait()
        live = span[0, 0] + span[0, 1]
        for k in range(4):
            for t in range(2):
                for stripe in range(stripes):
                    slot = stripe * kv_heads + (group ^ k)
                    for half in range(2):
                        at = (half * stripes + stripe) * run
                        outs[k][t, at : at + run, :] = turned[t, slot, half * run : (half + 1) * run]
        for slot in range(slots):
            position = (
                first + lax.broadcasted_iota(jnp.int32, (short, 1), 0) * stripes + slot // kv_heads
            )
            for t in range(2):
                slot_ref[slot, t] = jnp.where(
                    position < live, turned[t, slot].astype(jnp.float32), 0.0
                ).astype(jnp.bfloat16)

    piece = jax.ShapeDtypeStruct((2, rows, width), jnp.bfloat16)
    out_shape = [piece] * 4 + [jax.ShapeDtypeStruct((slots, 2, short, width), jnp.bfloat16)]
    return pl.pallas_call(
        kernel,
        in_specs=[pl.BlockSpec(memory_space=pltpu.HBM)] * 3,
        out_specs=[whole(out) for out in out_shape],
        out_shape=out_shape,
        scratch_shapes=[
            pltpu.SMEM(spans.shape, jnp.int32),
            pltpu.VMEM(keys.shape, jnp.bfloat16),
            pltpu.VMEM(keys.shape, jnp.bfloat16),
            pltpu.VMEM((2, slots, short, width), jnp.bfloat16),
            pltpu.SemaphoreType.DMA((3,)),
        ],
        compiler_params=small(62),
    )(spans, keys, values)


def pack_queries(queries):
    rows, head_count, width = queries.shape
    heads = head_count // 4

    def kernel(q_ref, *refs):
        outs, turned = refs[:4], refs[4]
        group = lax.axis_index("ctx") // 2
        turned[...] = jnp.swapaxes(q_ref[...], 0, 1)
        for k in range(4):
            outs[k][...] = turned[pl.ds((group ^ k) * heads, heads)]

    piece = jax.ShapeDtypeStruct((heads, rows, width), jnp.bfloat16)
    return pl.pallas_call(
        kernel,
        in_specs=[whole(queries)],
        out_specs=[whole(piece)] * 4,
        out_shape=[piece] * 4,
        scratch_shapes=[pltpu.VMEM((head_count, rows, width), jnp.bfloat16)],
        compiler_params=small(16),
    )(queries)


def join_heads(pieces):
    heads, rows, width = pieces[0].shape

    def kernel(*refs):
        ins, out, gathered = refs[:4], refs[4], refs[5]
        group = lax.axis_index("ctx") // 2
        for k in range(4):
            gathered[pl.ds((group ^ k) * heads, heads)] = ins[k][...]
        out[...] = jnp.swapaxes(gathered[...], 0, 1)

    out_shape = jax.ShapeDtypeStruct((rows, 4 * heads, width), jnp.bfloat16)
    return pl.pallas_call(
        kernel,
        in_specs=[whole(piece) for piece in pieces],
        out_specs=whole(out_shape),
        out_shape=out_shape,
        scratch_shapes=[pltpu.VMEM((4 * heads, rows, width), jnp.bfloat16)],
        compiler_params=small(16),
    )(*pieces)


def attend(which, queries, own, other, spans, stripes, grant):
    asked = len(which)
    members = len(own)
    heads, rows, width = queries[0].shape
    columns = heads * rows
    part_size = min(columns, 512)
    blocks = 2 * members
    log2_scale = 1.4426950408889634 / math.sqrt(width)

    def kernel(spans_ref, *refs):
        q_refs, kv_refs = refs[:asked], refs[asked : asked + blocks]
        o_refs = refs[asked + blocks : 2 * asked + blocks]
        scratch = refs[2 * asked + blocks :]
        q_in, values_in, key_blocks, values_t, query_t, mixed, peak, held, o_out, q_sem, k_sem, v_sem, o_sem = scratch
        step = pl.program_id(0)
        ctx = lax.axis_index("ctx")
        live = spans_ref[0, 0] + spans_ref[0, 1]
        block = ctx ^ flips[which[0]]
        for m in range(1, asked):
            block = jnp.where(step == m, ctx ^ flips[which[m]], block)
        theres = [ctx ^ flip for flip in flips] + [ctx ^ 1 ^ flip for flip in flips]
        q_copies = [
            pltpu.make_async_copy(q_refs[m], q_in.at[m], q_sem.at[m]) for m in range(asked)
        ]
        k_copies = [
            pltpu.make_async_copy(kv_refs[m].at[0], key_blocks.at[theres[m]], k_sem.at[m])
            for m in range(blocks)
        ]
        v_copies = [
            pltpu.make_async_copy(kv_refs[m].at[1], values_in.at[m], v_sem.at[m])
            for m in range(blocks)
        ]
        o_copies = [
            pltpu.make_async_copy(o_out.at[m], o_refs[m], o_sem.at[m]) for m in range(asked)
        ]

        @pl.when(step == 0)
        def _():
            for copy in (*v_copies, *q_copies, *k_copies):
                copy.start()
            values_t[:, width:] = jnp.ones_like(values_t[:, width:])
            for m in range(blocks):
                v_copies[m].wait()
                values_t[theres[m], :width] = values_in[m].T
            for copy in (*q_copies, *k_copies):
                copy.wait()

        @pl.when(block * rows >= live)
        def _():
            o_out[step] = jnp.zeros(o_out.shape[1:], o_out.dtype)

        @pl.when(block * rows < live)
        def _():
            for h in range(heads):
                query_t[:, h * rows : (h + 1) * rows] = q_in[step, h].T
            mixed[...] = jnp.zeros_like(mixed)
            peak[...] = jnp.full_like(peak, far_below)

            def scores(j, part):
                return jnp.dot(key_blocks[j], query_t[:, part], preferred_element_type=jnp.float32)

            def fold(s, j, part, depth=rows):
                old = peak[:, part]
                new = jnp.maximum(old, jnp.max(s, axis=0, keepdims=True))
                weights = jnp.exp2((s - new) * log2_scale)
                factor = jnp.exp2((old - new) * log2_scale)
                mixed[:, part] = mixed[:, part] * factor + jnp.dot(
                    values_t[j, :, :depth],
                    weights.astype(jnp.bfloat16),
                    preferred_element_type=jnp.float32,
                )
                peak[:, part] = new

            parts = [slice(a, a + part_size) for a in range(0, columns, part_size)]

            def earlier(slot, j):
                for part in parts:
                    s = held[slot, :, part]
                    held[1 - slot, :, part] = scores(j + 1, part)
                    fold(s, j, part)

            def diagonal(slot):
                half, run = rows // 2, rows // stripes // 2
                for a in range(0, columns, half):
                    part = slice(a, a + half)
                    depth = half if a % rows == 0 else rows
                    key_row = lax.broadcasted_iota(jnp.int32, (depth, half), 0)
                    within = lax.rem(key_row, half)
                    key_pos = key_row - within + lax.rem(within, run) * stripes + within // run
                    query_pos = lax.broadcasted_iota(jnp.int32, (depth, half), 1) + a % rows
                    s = jnp.where(key_pos <= query_pos, held[slot, :depth, part], far_below)
                    fold(s, block, part, depth)

            for part in parts:
                held[0, :, part] = scores(0, part)

            def two(t, carry):
                earlier(0, 2 * t)
                earlier(1, 2 * t + 1)
                return carry

            lax.fori_loop(0, block // 2, two, 0)

            @pl.when(lax.rem(block, 2) == 1)
            def _():
                earlier(0, block - 1)
                diagonal(1)

            @pl.when(lax.rem(block, 2) == 0)
            def _():
                diagonal(0)

            position = block * rows + lax.broadcasted_iota(jnp.int32, (rows, 1), 0)
            for h in range(heads):
                part = slice(h * rows, (h + 1) * rows)
                mixture = (mixed[:width, part] / mixed[width : width + 1, part]).T
                o_out[step, h] = jnp.where(position < live, mixture, 0.0).astype(jnp.bfloat16)

        for m in range(asked):

            @pl.when(step == m)
            def _():
                o_copies[m].start()

        @pl.when(step == asked - 1)
        def _():
            for copy in o_copies:
                copy.wait()

    arrays = (*queries, *own, *other)
    return pl.pallas_call(
        kernel,
        grid_spec=pltpu.PrefetchScalarGridSpec(
            num_scalar_prefetch=0,
            grid=(asked,),
            in_specs=[pl.BlockSpec(memory_space=pltpu.SMEM)]
            + [pl.BlockSpec(memory_space=pl.ANY)] * len(arrays),
            out_specs=[pl.BlockSpec(memory_space=pl.ANY)] * asked,
            scratch_shapes=[
                pltpu.VMEM((asked, heads, rows, width), jnp.bfloat16),
                pltpu.VMEM((blocks, rows, width), jnp.bfloat16),
                pltpu.VMEM((blocks, rows, width), jnp.bfloat16),
                pltpu.VMEM((blocks, width + 16, rows), jnp.bfloat16),
                pltpu.VMEM((width, columns), jnp.bfloat16),
                pltpu.VMEM((width + 16, columns), jnp.float32),
                pltpu.VMEM((1, columns), jnp.float32),
                pltpu.VMEM((2, rows, columns), jnp.float32),
                pltpu.VMEM((asked, heads, rows, width), jnp.bfloat16),
                pltpu.SemaphoreType.DMA((asked,)),
                pltpu.SemaphoreType.DMA((blocks,)),
                pltpu.SemaphoreType.DMA((blocks,)),
                pltpu.SemaphoreType.DMA((asked,)),
            ],
        ),
        out_shape=[jax.ShapeDtypeStruct(queries[0].shape, jnp.bfloat16)] * asked,
        compiler_params=pltpu.CompilerParams(
            dimension_semantics=("arbitrary",), vmem_limit_bytes=grant * 1024 * 1024
        ),
        cost_estimate=pl.CostEstimate(
            flops=4 * asked * members * heads * rows * rows * width,
            bytes_accessed=4 * rows * width * (asked * heads + 2 * members),
            transcendentals=asked * members * rows * rows * heads,
        ),
    )(spans, *arrays)


def take_blocks(array, order):
    def kernel(order_ref, in_ref, out_ref):
        for i in range(array.shape[0]):
            out_ref[i] = in_ref[order_ref[i]]

    return pl.pallas_call(
        kernel,
        in_specs=[pl.BlockSpec(memory_space=pltpu.SMEM), whole(array)],
        out_specs=whole(array),
        out_shape=jax.ShapeDtypeStruct(array.shape, array.dtype),
        compiler_params=small(8),
    )(order, array)


def place_rows(cache, held_rows):
    count, two, short, width = cache.shape
    blocks = count // held_rows
    out_shape = jax.ShapeDtypeStruct((held_rows, two, 1, blocks, short, width), cache.dtype)

    def kernel(in_ref, out_ref):
        for i in range(count):
            for t in range(two):
                out_ref[i % held_rows, t, 0, i // held_rows] = in_ref[i, t]

    return pl.pallas_call(
        kernel,
        in_specs=[whole(cache)],
        out_specs=whole(out_shape),
        out_shape=out_shape,
        compiler_params=small(8),
    )(cache)


def swap(array, axis):
    return lax.all_to_all(array, axis, split_axis=0, concat_axis=0, tiled=True)


def send(array, flip):
    return lax.ppermute(array, "ctx", route(flip))


def device_step(queries, keys, values, spans, partner):
    rows, _, width = queries.shape
    kv_heads = keys.shape[1]
    blocks = lax.axis_size("ctx")
    slots = lax.axis_size("prompt")
    stripes = slots // kv_heads

    by_slot = (rows // stripes, slots, width)
    *kv_out, slot_rows = pack_kv(keys.reshape(by_slot), values.reshape(by_slot), spans, kv_heads)
    own = [kv_out[0]] + [send(kv_out[k], flips[k]) for k in (1, 2, 3)]
    other_first = send(kv_out[0], 1)
    q_out = pack_queries(queries)
    q_own = [q_out[0]] + [send(q_out[k], flips[k]) for k in (1, 2, 3)]
    other = [other_first] + [send(own[k], 1) for k in (1, 2, 3)]

    by_prompt = swap(slot_rows, "prompt")
    by_row = take_blocks(by_prompt, partner)
    cache = swap(by_row, "ctx")
    cache = place_rows(cache, slots // blocks)

    done = [None] * 4
    for which, grant in (((1, 2), 62), ((3, 0), 62)):
        asked = [q_own[k] for k in which]
        for k, result in zip(which, attend(which, asked, own, other, spans, stripes, grant)):
            done[k] = result
    back = [done[0]] + [send(done[k], flips[k]) for k in (1, 2, 3)]
    return join_heads(back), cache


def solution(mesh):
    placed = P(("prompt", "ctx"), None, None)
    return jax.shard_map(
        device_step,
        mesh=mesh,
        in_specs=(placed, placed, placed, P("prompt", None), P()),
        out_specs=(placed, P("ctx", None, "prompt", None, None, None)),
        check_vma=False,
    )
```
